256 devices in a mesh: seq: 64 (over z, x, y_hi), head: 4 (over y_lo, core).
Axes of the slice: x: 4, y: 4 (y_hi: 2, y_lo: 2; y = y_hi * 2 + y_lo), z: 8, core: 2. Of those that a mesh axis runs over, the one named last changes fastest.
Arguments:
- queries: bfloat16 [16384, 24, 128], P('seq', 'head'), may hold values from -6 to 6
- key_vectors: bfloat16 [16384, 24, 128], P('seq', 'head'), may hold values from -6 to 6
- values: bfloat16 [16384, 24, 128], P('seq', 'head'), may hold values from -6 to 6
- out_grad: bfloat16 [16384, 24, 128], P('seq', 'head'), may hold values from -6 to 6
- ssm_input: bfloat16 [16384, 48, 128], P('seq', 'head'), may hold values from -6 to 6
- ssm_out_grad: bfloat16 [16384, 48, 128], P('seq', 'head'), may hold values from -1.5 to 1.5
- step_sizes: float32 [16384, 48], P('seq', 'head'), may hold values from 0 to 2, as said below
- decay_rates: float32 [48], P('head'), may hold values from -1 to 0, as said below
- skip_gains: float32 [48], P('head'), may hold values from 0.5 to 1.5
- bc_rows: bfloat16 [16384, 128], P('seq'), may hold values from -0.75 to 0.75
- saved_states: float32 [64, 48, 64, 128], P('seq', 'head'), may hold values from -6 to 6
Outputs:
- query_grad: bfloat16 [16384, 24, 128], P('seq', 'head')
- key_grad: bfloat16 [16384, 24, 128], P('seq', 'head')
- value_grad: bfloat16 [16384, 24, 128], P('seq', 'head')
- grad_inputs: bfloat16 [16384, 48, 128], P('seq', 'head')
- grad_steps: float32 [16384, 48], P('seq', 'head')
- grad_bc: float32 [16384, 128], P(('seq', 'head'))
- grad_decay: float32 [48], P('head')
- grad_skip: float32 [48], P('head')
The draws below stay inside these ranges and needn't reach their ends.
Inputs may be any that keep to these rules, and one draw needn't show every extreme that they name: `step_sizes`: positive. `decay_rates`: negative.
All inputs are finite; a program needn't handle non-finite values.
Results may differ from the reference program's by a relative error of at most 0.0095.
Values may be sent and summed in bfloat16 or wider, within the bound.
A program may use at most 192 MiB of HBM per device.

```python
import jax
import jax.numpy as jnp
from jax import lax

AHEADS = 24
HD = 128
STATE_SPACE_SETS = 48
MP = 128
NSTATE = 64
WINDOW = 1024
GROUP = 256
TOK_DEV = 256
SEQUENCE_LENGTH = 16384
SAVES = 64


def attention_pair(key):
    base_key = jax.random.fold_in(key, 11)
    key_q, key_k = jax.random.split(base_key, 2)
    shape_all = (SEQUENCE_LENGTH, AHEADS, HD)
    query_draw = jax.random.normal(key_q, shape_all, jnp.float32)
    key_draw = jax.random.normal(key_k, shape_all, jnp.float32)
    return (jnp.clip(query_draw, -6.0, 6.0), jnp.clip(key_draw, -6.0, 6.0))


def draw_queries(key, part):
    return attention_pair(key)[0].astype(jnp.bfloat16)


def draw_key_vectors(key, part):
    return attention_pair(key)[1].astype(jnp.bfloat16)


def draw_decay_rates(key, part):
    key_slow, key_fast, key_span = jax.random.split(jax.random.fold_in(key, 23), 3)
    slow_heads = jax.random.bernoulli(key_slow, 0.5, (STATE_SPACE_SETS,))
    fast_rate = -jax.random.uniform(key_fast, (STATE_SPACE_SETS,), jnp.float32, 0.4, 0.8)
    slow_rate = -jax.random.uniform(key_span, (STATE_SPACE_SETS,), jnp.float32, 0.5, 1.0) * (20.0 / SEQUENCE_LENGTH)
    return jnp.where(slow_heads, slow_rate, fast_rate)


def draw_step_sizes(key, part):
    key_rough, key_block, key_place, key_amount = jax.random.split(jax.random.fold_in(key, 31), 4)
    approximate_guess = jax.random.uniform(key_rough, (SEQUENCE_LENGTH, STATE_SPACE_SETS), jnp.float32, 0.5, 1.5)
    segmented_lines = jnp.exp(jax.random.uniform(key_block, (SEQUENCE_LENGTH // TOK_DEV, 1, STATE_SPACE_SETS), jnp.float32, -0.4, 0.4))
    segmented_lines = jnp.broadcast_to(segmented_lines, (SEQUENCE_LENGTH // TOK_DEV, TOK_DEV, STATE_SPACE_SETS)).reshape(SEQUENCE_LENGTH, STATE_SPACE_SETS)
    location_series = jax.random.randint(key_place, (3, STATE_SPACE_SETS), 0, SEQUENCE_LENGTH)
    quantity_series = jax.random.uniform(key_amount, (3, STATE_SPACE_SETS), jnp.float32, 2.0, 6.0)
    vertical_position = jnp.arange(SEQUENCE_LENGTH)[:, None]
    packet_clusters = jnp.zeros((SEQUENCE_LENGTH, STATE_SPACE_SETS), jnp.float32)
    for numeric_quantity in range(3):
        packet_clusters = packet_clusters + jnp.where(vertical_position == location_series[numeric_quantity][None, :], quantity_series[numeric_quantity][None, :], 0.0)
    return 0.05 * approximate_guess * segmented_lines + 0.05 * packet_clusters


def block_scale(key, shape, cuts, least, high):
    def one(axis_at, parts):
        draws = jax.random.uniform(jax.random.fold_in(jax.random.fold_in(key, 6), axis_at), (parts,), jnp.float32, least / len(cuts), high / len(cuts))
        return jnp.repeat(jnp.exp(draws), shape[axis_at] // parts).reshape((-1,) + (1,) * (len(shape) - axis_at - 1))

    factor_of = one(*cuts[0])
    for cut in cuts[1:]:
        factor_of = factor_of * one(*cut)
    return factor_of


def bell_draw(own_key, shape, width, limit, cuts=(), kind=jnp.bfloat16):
    drawn = width * jax.random.normal(own_key, shape, jnp.float32)
    if cuts:
        drawn = drawn * block_scale(own_key, shape, cuts, -0.22, 0.18)
    return jnp.clip(drawn, -limit, limit).astype(kind)


def setup_inputs(seed: int = 0) -> dict:
    streams_of = jax.random.split(jax.random.key(seed), 12)
    queries = draw_queries(jax.random.fold_in(streams_of[11], 71), 0)
    key_vectors = draw_key_vectors(jax.random.fold_in(streams_of[11], 71), 0)
    values = bell_draw(streams_of[2], (SEQUENCE_LENGTH, AHEADS, HD), 1.0, 6.0, ((0, 64), (1, 4)))
    out_grad = bell_draw(streams_of[3], (SEQUENCE_LENGTH, AHEADS, HD), 1.0, 6.0, ((0, 64), (1, 4)))
    ssm_input = bell_draw(streams_of[4], (SEQUENCE_LENGTH, STATE_SPACE_SETS, MP), 1.0, 6.0, ((0, 64), (1, 4)))
    ssm_out_grad = bell_draw(streams_of[5], (SEQUENCE_LENGTH, STATE_SPACE_SETS, MP), 0.25, 1.5, ((0, 64), (1, 4)))
    step_sizes = draw_step_sizes(jax.random.fold_in(streams_of[11], 71), 0)
    decay_rates = draw_decay_rates(jax.random.fold_in(streams_of[11], 71), 0)
    skip_gains = jnp.clip(0.5 + 1.0 * jax.random.uniform(streams_of[8], (STATE_SPACE_SETS,), jnp.float32) ** block_scale(streams_of[8], (STATE_SPACE_SETS,), ((0, 4),), -0.2, 0.2), 0.5, 1.5)
    bc_rows = bell_draw(streams_of[9], (SEQUENCE_LENGTH, 2 * NSTATE), 0.125, 0.75, ((0, 64),))
    saved_states = bell_draw(streams_of[10], (SAVES, STATE_SPACE_SETS, NSTATE, MP), 1.0, 6.0, ((0, 64), (1, 4)), jnp.float32)
    return {"queries": queries, "key_vectors": key_vectors, "values": values, "out_grad": out_grad, "ssm_input": ssm_input, "ssm_out_grad": ssm_out_grad, "step_sizes": step_sizes, "decay_rates": decay_rates, "skip_gains": skip_gains, "bc_rows": bc_rows, "saved_states": saved_states}


TOP_PRECISION = lax.Precision.HIGHEST

def attention_grads(queries, key_vectors, values, out_grad):
    count = TOK_DEV
    extent = WINDOW + TOK_DEV
    blocks_total = SEQUENCE_LENGTH // TOK_DEV
    scaling_factor = HD ** (-0.5)
    padding = jnp.zeros((WINDOW, AHEADS, HD), queries.dtype)
    keys_pad = jnp.concatenate([padding, key_vectors], axis=0)
    values_pad = jnp.concatenate([padding, values], axis=0)
    row_ids = lax.broadcasted_iota(jnp.int32, (count, extent), 0)
    col_ids = lax.broadcasted_iota(jnp.int32, (count, extent), 1)

    def block_step(carry, block_id):
        key_acc, value_acc = carry
        begin = (block_id * count).astype(jnp.int32)
        query_tile = lax.dynamic_slice_in_dim(queries, begin, count, 0).astype(jnp.float32)
        gradient_block = lax.dynamic_slice_in_dim(out_grad, begin, count, 0).astype(jnp.float32)
        key_tile = lax.dynamic_slice_in_dim(keys_pad, begin, extent, 0).astype(jnp.float32)
        value_tile = lax.dynamic_slice_in_dim(values_pad, begin, extent, 0).astype(jnp.float32)
        usable = (col_ids > row_ids) & (col_ids <= WINDOW + row_ids) & (col_ids + begin >= WINDOW)
        score_matrix = jnp.einsum('uoh,soh->ous', query_tile, key_tile, precision=TOP_PRECISION) * scaling_factor
        score_matrix = jnp.where(usable[None], score_matrix, -jnp.inf)
        row_max = lax.optimization_barrier(jnp.max(score_matrix, axis=2, keepdims=True))
        log_total = row_max + jnp.log(lax.optimization_barrier(jnp.sum(jnp.exp(score_matrix - row_max), axis=2, keepdims=True)))
        probs = jnp.exp(score_matrix - log_total)
        probs_reduced = probs.astype(jnp.bfloat16).astype(jnp.float32)
        probs_gradient = jnp.einsum('uoh,soh->ous', gradient_block, value_tile, precision=TOP_PRECISION)
        delta_row = lax.optimization_barrier(jnp.sum(probs * probs_gradient, axis=2, keepdims=True))
        scores_gradient = (probs * (probs_gradient - delta_row) * scaling_factor).astype(jnp.bfloat16).astype(jnp.float32)
        query_gradient = jnp.einsum('uzs,suy->zuy', scores_gradient, key_tile, precision=TOP_PRECISION)
        key_gradient = jnp.einsum('wut,uwc->twc', scores_gradient, query_tile, precision=TOP_PRECISION)
        value_gradient = jnp.einsum('wut,uwc->twc', probs_reduced, gradient_block, precision=TOP_PRECISION)
        key_acc = lax.dynamic_update_slice_in_dim(key_acc, lax.dynamic_slice_in_dim(key_acc, begin, extent, 0) + key_gradient, begin, 0)
        value_acc = lax.dynamic_update_slice_in_dim(value_acc, lax.dynamic_slice_in_dim(value_acc, begin, extent, 0) + value_gradient, begin, 0)
        return ((key_acc, value_acc), query_gradient.astype(jnp.bfloat16))
    zero_acc = jnp.zeros((WINDOW + SEQUENCE_LENGTH, AHEADS, HD), jnp.float32)
    (key_acc, value_acc), q_grads = lax.scan(block_step, (zero_acc, zero_acc), jnp.arange(blocks_total, dtype=jnp.int32))
    query_grad = q_grads.reshape(SEQUENCE_LENGTH, AHEADS, HD)
    return (query_grad, key_acc[WINDOW:].astype(jnp.bfloat16), value_acc[WINDOW:].astype(jnp.bfloat16))

def group_loss(inputs_part, steps_part, bc_part, decay_rates, skip_gains, start_state, incoming, out_part):
    log_decay = steps_part * decay_rates[None, :]
    cumulative = jnp.cumsum(log_decay, axis=0)
    last_sum = cumulative[-1]
    b_rows = bc_part[:, :NSTATE]
    c_rows = bc_part[:, NSTATE:]
    row_ids = lax.broadcasted_iota(jnp.int32, (GROUP, GROUP), 0)
    col_ids = lax.broadcasted_iota(jnp.int32, (GROUP, GROUP), 1)
    in_lower = (col_ids <= row_ids)[None]
    spread = cumulative.T[:, :, None] - cumulative.T[:, None, :]
    lower_decay = jnp.where(in_lower, jnp.exp(jnp.where(in_lower, spread, 0.0)), 0.0)
    inner_cb = jnp.dot(c_rows, b_rows.T, precision=TOP_PRECISION)
    driven = steps_part[:, :, None] * inputs_part
    outputs = jnp.exp(cumulative)[:, :, None] * jnp.einsum('tn,hnp->thp', c_rows, start_state, precision=TOP_PRECISION)
    outputs = outputs + jnp.einsum('hts,shp->thp', lower_decay * inner_cb[None], driven, precision=TOP_PRECISION)
    outputs = outputs + skip_gains[None, :, None] * inputs_part
    tail_decay = jnp.exp(last_sum[None, :] - cumulative)
    final_state = jnp.exp(last_sum)[:, None, None] * start_state
    final_state = final_state + jnp.einsum('shp,sn->hnp', driven * tail_decay[:, :, None], b_rows, precision=TOP_PRECISION)
    return jnp.sum(outputs * out_part) + jnp.sum(incoming * final_state)

def ssm_grads(ssm_input, ssm_out_grad, step_sizes, decay_rates, skip_gains, bc_rows, saved_states):
    pieces = SEQUENCE_LENGTH // GROUP
    inputs_f = ssm_input.astype(jnp.float32).reshape(pieces, GROUP, STATE_SPACE_SETS, MP)
    grads_f = ssm_out_grad.astype(jnp.float32).reshape(pieces, GROUP, STATE_SPACE_SETS, MP)
    steps_f = step_sizes.reshape(pieces, GROUP, STATE_SPACE_SETS)
    bc_f = bc_rows.astype(jnp.float32).reshape(pieces, GROUP, 2 * NSTATE)
    gradient = jax.grad(group_loss, argnums=(0, 1, 2, 3, 4, 5))

    def backward_step(carry, item):
        incoming, decay_sum, skip_sum = carry
        inputs_part, out_part, steps_part, bc_part, start_state = item
        g_inputs, g_steps, g_bc, g_decay, g_skip, g_start = gradient(inputs_part, steps_part, bc_part, decay_rates, skip_gains, start_state, incoming, out_part)
        return ((g_start, decay_sum + g_decay, skip_sum + g_skip), (g_inputs, g_steps, g_bc))
    initial = (jnp.zeros((STATE_SPACE_SETS, NSTATE, MP), jnp.float32), jnp.zeros((STATE_SPACE_SETS,), jnp.float32), jnp.zeros((STATE_SPACE_SETS,), jnp.float32))
    (unused, decay_sum, skip_sum), (g_inputs, g_steps, g_bc) = lax.scan(backward_step, initial, (inputs_f, grads_f, steps_f, bc_f, saved_states), reverse=True)
    grad_inputs = g_inputs.reshape(SEQUENCE_LENGTH, STATE_SPACE_SETS, MP).astype(jnp.bfloat16)
    grad_steps = g_steps.reshape(SEQUENCE_LENGTH, STATE_SPACE_SETS)
    grad_bc = g_bc.reshape(SEQUENCE_LENGTH, 2 * NSTATE)
    return (grad_inputs, grad_steps, grad_bc, decay_sum, skip_sum)

def reference(queries, key_vectors, values, out_grad, ssm_input, ssm_out_grad, step_sizes, decay_rates, skip_gains, bc_rows, saved_states):
    query_grad, key_grad, value_grad = attention_grads(queries, key_vectors, values, out_grad)
    grad_inputs, grad_steps, grad_bc, grad_decay, grad_skip = ssm_grads(ssm_input, ssm_out_grad, step_sizes, decay_rates, skip_gains, bc_rows, saved_states)
    return (query_grad, key_grad, value_grad, grad_inputs, grad_steps, grad_bc, grad_decay, grad_skip)
```

```python
import functools
import math

import jax
import jax.numpy as jnp
from jax import lax
from jax.experimental import pallas as pl
from jax.experimental.pallas import tpu as pltpu
from jax.sharding import Mesh
from jax.sharding import PartitionSpec as P

NSTATE = 64
SEQ = ("seq_0", "seq_1", "seq_2")
SEQ_HEAD = ("seq_0", "seq_1", "seq_2", "head")
AXES = ("seq_0", "seq_1", "seq_2", "head")
MESH = pl.DeviceIdType.MESH
HIGHEST = lax.Precision.HIGHEST
NEG = -1e30
UNIT = 256
HD = 128
SCALE = HD**-0.5
SCALE2 = SCALE * math.log2(math.e)
PLANE = 8
ZS = 8
XS = 4
PAIRS = ZS * XS
BF = jnp.bfloat16
F32 = jnp.float32


def dot(a, b, dims, precision=None):
    return lax.dot_general(a, b, (dims, ((), ())), precision=precision, preferred_element_type=F32)


def nn(a, b, precision=None):
    return dot(a, b, ((1,), (0,)), precision)


def nt(a, b):
    return dot(a, b, ((1,), (1,)))


def tn(a, b):
    return dot(a, b, ((0,), (0,)))


def kernel(
    k6, v6, q6, g6, xs, dy, st, rates, skips, b_in, c_in, s0,
    dq6, dk6, dv6, gx, gst, gbc, gtot,
    kv, qg, stat, og, tscr, dscr,
    lb, sb, lrow, rrow, skr, whr, cbt, wsum, gb_acc, gc_acc, g0, ec,
    car, plin, eplane, pplane, zt, zin, incout, inc,
    gbcl, gbin, tsrc, tpl, tz_src, tz,
    yin_s, yin_r, x1_s, x1_r, x2_s, x2_r, st_s, st_r, yo_s, yo_r,
    s1_s, s1_r, s2_s, s2_r, s3_s, s3_r, hb_s, hb_r, ta_s, ta_r, tb_s, tb_r,
):
    z, x, yh, hd = [lax.axis_index(a) for a in AXES]
    yl, core = hd // 2, hd % 2
    j = z * XS + x
    m = x * 2 + yh
    other = (1 - yl) * 2 + core
    heads = xs.shape[0]

    def at_pair(d):
        t = (j + d + PAIRS) % PAIRS
        return (t // XS, t % XS, yh, hd)

    def at_plane(mm):
        return (z, mm // 2, mm % 2, hd)

    def at_z(zz):
        return (zz, x, yh, hd)

    def at_head(hh):
        return (z, x, yh, hh)

    def at_y(k):
        return (z, x, k, other)

    def rcopy(src, dst, ss, rs, to):
        return pltpu.make_async_remote_copy(
            src_ref=src, dst_ref=dst, send_sem=ss, recv_sem=rs, device_id=to, device_id_type=MESH
        )

    peers = [at_y(0), at_y(1), at_pair(1), at_pair(-1), at_pair(2), at_pair(-2)]
    peers += [at_plane((m + o) % PLANE) for o in range(1, PLANE)]
    peers += [at_z((z + o) % ZS) for o in range(1, ZS)]
    peers += [at_head((hd + o) % 4) for o in range(1, 4)]
    barrier = pltpu.get_barrier_semaphore()
    for p in peers:
        pl.semaphore_signal(barrier, inc=1, device_id=p, device_id_type=MESH)
    pl.semaphore_wait(barrier, len(peers))

    sources = ((k6, v6), (q6, g6))
    lands = ((kv, 4), (qg, 0))

    def y_in(h, w, t, k, sender):
        buf, base = lands[w]
        return rcopy(
            sources[w][t].at[3 * k + h], buf.at[base + sender, h, t],
            yin_s.at[w, h, t, k], yin_r.at[w, h, t, sender], at_y(k),
        )

    def start_y_in(h):
        for w in range(2):
            for t in range(2):
                for k in range(2):
                    y_in(h, w, t, k, yh).start()

    def wait_y_in(h, w):
        for t in range(2):
            for k in range(2):
                y_in(h, w, t, k, k).wait_recv()

    def hop(n, w, h):
        if w == 0:
            src, dst, to = (kv.at[pl.ds(6 - 2 * n, 2), h], kv.at[pl.ds(4 - 2 * n, 2), h], at_pair(1))
        else:
            src, dst, to = (qg.at[pl.ds(2 * n - 2, 2), h], qg.at[pl.ds(2 * n, 2), h], at_pair(-1))
        ss, rs = ((x1_s, x1_r), (x2_s, x2_r))[n - 1]
        return rcopy(src, dst, ss.at[w, h], rs.at[w, h], to)

    def stat_copy(h, d):
        return rcopy(
            stat.at[pl.ds(0, 2), h], stat.at[pl.ds(2 * d, 2), h],
            st_s.at[d - 1, h], st_r.at[d - 1, h], at_pair(-d),
        )

    outs = (dq6, dk6, dv6)

    def y_out(n, h, i, sender):
        return rcopy(
            og.at[n, h, i], outs[n].at[3 * sender + h],
            yo_s.at[n, h, i], yo_r.at[n, h, sender], at_y(i),
        )

    def s1(o, to_m, from_m):
        return rcopy(
            car.at[:, pl.ds(pl.multiple_of(8 * to_m, 8), 8), :], plin.at[from_m],
            s1_s.at[o - 1], s1_r.at[o - 1], at_plane(to_m),
        )

    def s2(o, to_z, from_z):
        return rcopy(zt, zin.at[from_z], s2_s.at[o - 1], s2_r.at[o - 1], at_z(to_z))

    def s3(o, to_m, from_m):
        return rcopy(
            incout.at[to_m], inc.at[:, pl.ds(pl.multiple_of(8 * from_m, 8), 8), :],
            s3_s.at[o - 1], s3_r.at[o - 1], at_plane(to_m),
        )

    def hb(o, to_h, from_h):
        return rcopy(
            gbcl.at[pl.ds(pl.multiple_of(64 * to_h, 64), 64), :], gbin.at[from_h],
            hb_s.at[o - 1], hb_r.at[o - 1], at_head(to_h),
        )

    def ta(o, to_m, from_m):
        return rcopy(tsrc, tpl.at[from_m], ta_s.at[o - 1], ta_r.at[o - 1], at_plane(to_m))

    def tb(o, to_z, from_z):
        return rcopy(tz_src, tz.at[from_z], tb_s.at[o - 1], tb_r.at[o - 1], at_z(to_z))

    def start_all(make, mine, count):
        for o in range(1, count):
            make(o, (mine + o) % count, mine).start()

    def recv_all(make, mine, count):
        for o in range(1, count):
            make(o, mine, (mine + count - o) % count).wait_recv()

    def sent_all(make, mine, count):
        for o in range(1, count):
            make(o, (mine + o) % count, mine).wait_send()

    rowi = lax.broadcasted_iota(jnp.int32, (UNIT, UNIT), 0)
    coli = lax.broadcasted_iota(jnp.int32, (UNIT, UNIT), 1)

    start_y_in(0)
    start_y_in(1)
    start_y_in(2)
    steps = st[...]
    inclusive = (coli <= rowi).astype(F32)
    lcol = nn(inclusive, steps * rates[...], HIGHEST)
    lrow[...] = lcol.T
    decays = jnp.exp(lcol[UNIT - 1 : UNIT, :])
    for h in range(heads):
        lb[h] = jnp.broadcast_to(lcol[:, h : h + 1], (UNIT, HD))
        sb[h] = jnp.broadcast_to(steps[:, h : h + 1], (UNIT, HD))

    def summary(h, carry):
        scaled = (dy[h].astype(F32) * jnp.exp(lb[h])).astype(BF)
        car[h] = tn(c_in[...], scaled)
        return carry

    lax.fori_loop(0, heads, summary, 0)
    car[heads] = jnp.broadcast_to(decays, (NSTATE, HD))
    start_all(s1, m, PLANE)
    plin[m] = car[:, pl.ds(pl.multiple_of(8 * m, 8), 8), :]

    cbt[...] = nt(b_in[...], c_in[...])

    def send_own(h):
        for w in range(2):
            wait_y_in(h, w)
            hop(1, w, h).start()

    def send_next(h):
        for w in range(2):
            hop(1, w, h).wait_recv()
            hop(2, w, h).start()

    send_own(0)

    recv_all(s1, m, PLANE)
    acc = [jnp.zeros((8, HD), F32)] * heads
    prod = [jnp.ones((8, HD), F32)] * heads
    tile_prod = jnp.ones((8, HD), F32)
    for mm in reversed(range(PLANE)):
        tile = plin[mm, heads]
        tile_prod = tile_prod * tile
        for h in range(heads):
            eplane[mm, h] = acc[h]
            pplane[mm, h] = prod[h]
            decay = jnp.broadcast_to(tile[:, h : h + 1], (8, HD))
            acc[h] = plin[mm, h] + decay * acc[h]
            prod[h] = prod[h] * decay
    for h in range(heads):
        zt[h] = acc[h]
    zt[heads] = tile_prod
    start_all(s2, z, ZS)
    zin[z] = zt[...]

    send_own(1)
    send_next(0)

    recv_all(s2, z, ZS)
    acc = [jnp.zeros((8, HD), F32)] * heads
    for zz in reversed(range(1, ZS)):
        tile = zin[zz, heads]
        for h in range(heads):
            decay = jnp.broadcast_to(tile[:, h : h + 1], (8, HD))
            acc[h] = jnp.where(zz > z, zin[zz, h] + decay * acc[h], acc[h])
    for mm in range(PLANE):
        for h in range(heads):
            incout[mm, h] = eplane[mm, h] + pplane[mm, h] * acc[h]
    start_all(s3, m, PLANE)
    inc[:, pl.ds(pl.multiple_of(8 * m, 8), 8), :] = incout[m]

    send_own(2)
    send_next(1)

    recv_all(s3, m, PLANE)
    for ref in (rrow, skr, whr, wsum, gb_acc, gc_acc, g0, ec, tsrc):
        ref[...] = jnp.zeros_like(ref)
    lanes = lax.broadcasted_iota(jnp.int32, (UNIT, HD), 1)

    def wide(t):
        return jnp.concatenate([t, t], axis=1)

    def grads(h, carry):
        b_rows, c_rows = (b_in[...], c_in[...])
        lc, sc = (lb[h], sb[h])
        lr = lrow[pl.ds(h, 1), :]
        x_h, dy_h = (xs[h], dy[h])
        cb = cbt[...]
        decay = jnp.exp(jnp.where(coli >= rowi, lr - wide(lc), NEG))
        crossed = decay * nt(x_h, dy_h)
        weighted = crossed * wide(sc)
        wsum[...] += weighted
        rrow[pl.ds(h, 1), :] = jnp.sum(weighted * cb, axis=0, keepdims=True)
        paired = crossed * cb
        mixing = (decay * cb).astype(BF)
        tail = jnp.exp(lc[UNIT - 1 : UNIT, :] - lc)
        weights = jnp.exp(lc)
        inc_f, s0_f = (inc[h], s0[h])
        inc_h, s0_h = (inc_f.astype(BF), s0_f.astype(BF))
        dy_f = dy_h.astype(F32)
        driven_grad = nn(mixing, dy_h) + tail * nn(b_rows, inc_h)
        gx[h] = (sc * driven_grad + skips[h] * dy_f).astype(BF)
        late = nt(x_h, inc_h) * tail[:, :NSTATE]
        gb_acc[...] += sc[:, :NSTATE] * late
        early = nt(dy_h, s0_h) * weights[:, :NSTATE]
        gc_acc[...] += early
        own = jnp.sum(paired[:, :HD] + paired[:, HD:], axis=1, keepdims=True)
        own = own + jnp.sum(late * b_rows.astype(F32), axis=1, keepdims=True)
        first = jnp.sum(early * c_rows.astype(F32), axis=1, keepdims=True)
        here = lanes == h
        g0[...] += jnp.where(here, own, 0.0)
        ec[...] += jnp.where(here, first, 0.0)
        skr[pl.ds(h, 1), :] = jnp.sum(dy_f * x_h.astype(F32), axis=0, keepdims=True)
        whr[pl.ds(h, 1), :] = jnp.sum(inc_f * s0_f, axis=0, keepdims=True)
        return carry

    lax.fori_loop(0, heads, grads, 0)
    w_all = wsum[...]
    gb_all = gb_acc[...] + nn(w_all, c_in[...].astype(F32), HIGHEST)
    gc_all = gc_acc[...] + nn(w_all.T, b_in[...].astype(F32), HIGHEST)
    gbcl[...] = jnp.concatenate([gb_all, gc_all], axis=1)
    start_all(hb, hd, 4)
    gbin[hd] = gbcl[pl.ds(pl.multiple_of(64 * hd, 64), 64), :]
    steps = st[...]
    early_all = ec[...]
    change = steps * g0[...] - rrow[...].T - early_all
    strict = (coli < rowi).astype(F32)
    whole = decays * jnp.sum(whr[...].T, axis=0, keepdims=True)
    grad_log = nn(strict, change, HIGHEST) + (jnp.sum(early_all, axis=0, keepdims=True) + whole)
    gst[...] = g0[...] + rates[...] * grad_log
    tsrc[0:1, :] = jnp.sum(steps * grad_log, axis=0, keepdims=True)
    tsrc[1:2, :] = jnp.sum(skr[...].T, axis=0, keepdims=True)
    start_all(ta, m, PLANE)
    tpl[m] = tsrc[...]

    send_next(2)

    def window(h):
        def block(i, carry):
            q, g = (qg[i, h, 0], qg[i, h, 1])
            top = None
            for u in range(5):
                s = nt(kv[i + u, h, 0], q) * SCALE2
                if u == 0:
                    s = jnp.where(rowi > coli, s, NEG)
                if u == 4:
                    s = jnp.where(rowi <= coli, s, NEG)
                else:
                    s = s + jnp.where(2 * j + i + u >= 4, 0.0, NEG)
                tscr[u] = s
                best = jnp.max(s, axis=0, keepdims=True)
                top = best if top is None else jnp.maximum(top, best)
            total = jnp.zeros((1, UNIT), F32)
            delta = jnp.zeros((1, UNIT), F32)
            for u in range(5):
                e = jnp.exp2(tscr[u] - top)
                dp = nt(kv[i + u, h, 1], g)
                total = total + jnp.sum(e, axis=0, keepdims=True)
                delta = delta + jnp.sum(e * dp, axis=0, keepdims=True)
                tscr[u] = e
                dscr[u] = dp
            inverse = 1.0 / total
            delta = delta * inverse
            out = jnp.zeros((HD, UNIT), F32)
            for u in range(5):
                ds = (tscr[u] * (dscr[u] - delta)).astype(BF)
                out = out + tn(kv[i + u, h, 0], ds)
            og[0, h, i] = (out * (inverse * SCALE)).T.astype(BF)
            stat[i, h, 0:1, :] = top + jnp.log2(total)
            stat[i, h, 1:2, :] = delta
            return carry

        lax.fori_loop(0, 2, block, 0)

    def key_pass(h):
        def block(i, carry):
            k, v = (kv[4 + i, h, 0], kv[4 + i, h, 1])
            dk = jnp.zeros((UNIT, HD), F32)
            dv = jnp.zeros((UNIT, HD), F32)
            for u in range(5):
                q, g = (qg[i + u, h, 0], qg[i + u, h, 1])
                s = nt(k, q) * SCALE2 - stat[i + u, h, 0:1, :]
                if u == 0:
                    s = jnp.where(coli >= rowi, s, NEG)
                else:
                    s = s + jnp.where(2 * j + i + u < 2 * PAIRS, 0.0, NEG)
                if u == 4:
                    s = jnp.where(coli < rowi, s, NEG)
                p = jnp.exp2(s)
                dv = dv + nn(p.astype(BF), g)
                ds = (p * (nt(v, g) - stat[i + u, h, 1:2, :])).astype(BF)
                dk = dk + nn(ds, q)
            og[1, h, i] = (dk * SCALE).astype(BF)
            og[2, h, i] = dv.astype(BF)
            return carry

        lax.fori_loop(0, 2, block, 0)

    def windows(h):
        hop(2, 0, h).wait_recv()
        window(h)
        for d in (1, 2):
            stat_copy(h, d).start()
        for i in range(2):
            y_out(0, h, i, yh).start()

    def keys(h):
        hop(2, 1, h).wait_recv()
        for d in (1, 2):
            stat_copy(h, d).wait_recv()
        key_pass(h)
        for n in (1, 2):
            for i in range(2):
                y_out(n, h, i, yh).start()

    for h in range(3):
        for ref in (stat,):
            ref[0:2, h] = jnp.zeros((2, 8, UNIT), F32)
    windows(0)
    windows(1)
    keys(0)

    recv_all(ta, m, PLANE)
    plane_sum = tpl[0]
    for mm in range(1, PLANE):
        plane_sum = plane_sum + tpl[mm]
    tz_src[...] = plane_sum
    start_all(tb, z, ZS)
    tz[z] = plane_sum

    windows(2)
    keys(1)

    recv_all(hb, hd, 4)
    gbc[...] = ((gbin[0] + gbin[1]) + gbin[2]) + gbin[3]
    recv_all(tb, z, ZS)
    total = tz[0]
    for zz in range(1, ZS):
        total = total + tz[zz]
    gtot[...] = total

    keys(2)

    for h in range(3):
        for n in range(3):
            for i in range(2):
                y_out(n, h, i, i).wait_recv()
    for h in range(3):
        for w in range(2):
            for t in range(2):
                for k in range(2):
                    y_in(h, w, t, k, yh).wait_send()
            for n in (1, 2):
                hop(n, w, h).wait_send()
        for d in (1, 2):
            stat_copy(h, d).wait_send()
        for n in range(3):
            for i in range(2):
                y_out(n, h, i, yh).wait_send()
    sent_all(s1, m, PLANE)
    sent_all(s2, z, ZS)
    sent_all(s3, m, PLANE)
    sent_all(hb, hd, 4)
    sent_all(ta, m, PLANE)
    sent_all(tb, z, ZS)


def shards(
    queries, key_vectors, values, out_grad, ssm_input, ssm_out_grad,
    step_sizes, decay_rates, skip_gains, bc_rows, saved_states,
):
    heads = ssm_input.shape[1]
    by_head = [
        jnp.transpose(t, (1, 0, 2))
        for t in (key_vectors, values, queries, out_grad, ssm_input, ssm_out_grad)
    ]
    steps = jnp.pad(step_sizes, ((0, 0), (0, HD - heads)))
    rates = jnp.pad(decay_rates, (0, HD - heads))[None, :]
    vmem = pl.BlockSpec(memory_space=pltpu.VMEM)
    smem = pl.BlockSpec(memory_space=pltpu.SMEM)

    def shape(s, t=F32):
        return jax.ShapeDtypeStruct(s, t)

    def scratch(s, t=F32):
        return pltpu.VMEM(s, t)

    dma = pltpu.SemaphoreType.DMA
    wide = (heads, UNIT, HD)
    tile = (8, HD)
    out = pl.pallas_call(
        kernel,
        name="mixers",
        out_shape=[
            shape((6, UNIT, HD), BF), shape((6, UNIT, HD), BF), shape((6, UNIT, HD), BF),
            shape(wide, BF), shape((UNIT, HD)), shape((UNIT // 4, HD)), shape(tile),
        ],
        in_specs=[vmem] * 8 + [smem] + [vmem] * 3,
        out_specs=[vmem] * 7,
        scratch_shapes=[
            scratch((6, 3, 2, UNIT, HD), BF), scratch((6, 3, 2, UNIT, HD), BF),
            scratch((6, 3, 8, UNIT)), scratch((3, 3, 2, UNIT, HD), BF),
            scratch((5, UNIT, UNIT)), scratch((5, UNIT, UNIT)),
            scratch(wide), scratch(wide), scratch((HD, UNIT)), scratch((HD, UNIT)),
            scratch((HD, HD)), scratch((HD, HD)), scratch((UNIT, UNIT)), scratch((UNIT, UNIT)),
            scratch((UNIT, NSTATE)), scratch((UNIT, NSTATE)), scratch((UNIT, HD)), scratch((UNIT, HD)),
            scratch((heads + 1, NSTATE, HD)), scratch((PLANE, heads + 1, *tile)),
            scratch((PLANE, heads, *tile)), scratch((PLANE, heads, *tile)),
            scratch((heads + 1, *tile)), scratch((ZS, heads + 1, *tile)),
            scratch((PLANE, heads, *tile)), scratch((heads, NSTATE, HD)),
            scratch((UNIT, HD)), scratch((4, UNIT // 4, HD)),
            scratch(tile), scratch((PLANE, *tile)), scratch(tile), scratch((ZS, *tile)),
            dma((2, 3, 2, 2)), dma((2, 3, 2, 2)), dma((2, 3)), dma((2, 3)), dma((2, 3)), dma((2, 3)),
            dma((2, 3)), dma((2, 3)), dma((3, 3, 2)), dma((3, 3, 2)),
            dma((7,)), dma((7,)), dma((7,)), dma((7,)), dma((7,)), dma((7,)),
            dma((3,)), dma((3,)), dma((7,)), dma((7,)), dma((7,)), dma((7,)),
        ],
        compiler_params=pltpu.CompilerParams(
            collective_id=0, has_side_effects=True, vmem_limit_bytes=60 * 1024 * 1024
        ),
    )(
        *by_head, steps, rates, skip_gains, bc_rows[:, :NSTATE], bc_rows[:, NSTATE:], saved_states[0]
    )
    dq6, dk6, dv6, gx, gst, gbc, gtot = out
    return (
        jnp.transpose(dq6, (1, 0, 2)),
        jnp.transpose(dk6, (1, 0, 2)),
        jnp.transpose(dv6, (1, 0, 2)),
        jnp.transpose(gx, (1, 0, 2)),
        gst[:, :heads],
        gbc,
        gtot[0, :heads],
        gtot[1, :heads],
    )


def solution(mesh):
    torus = Mesh(mesh.devices.reshape(ZS, XS, 2, mesh.shape["head"]), AXES)
    token_head = P(SEQ, "head", None)
    in_specs = (token_head,) * 6 + (
        P(SEQ, "head"), P("head"), P("head"), P(SEQ, None), P(SEQ, "head", None, None),
    )
    out_specs = (token_head,) * 4 + (P(SEQ, "head"), P(SEQ_HEAD, None), P("head"), P("head"))
    return jax.shard_map(shards, mesh=torus, in_specs=in_specs, out_specs=out_specs, check_vma=False)
```

```python
import functools
import math

import jax
import jax.numpy as jnp
from jax import lax
from jax.experimental import pallas as pl
from jax.experimental.pallas import tpu as pltpu
from jax.sharding import Mesh
from jax.sharding import PartitionSpec as P

NSTATE = 64
SEQ = ("seq_0", "seq_1", "seq_2")
SEQ_HEAD = ("seq_0", "seq_1", "seq_2", "head")
AXES = ("seq_0", "seq_1", "seq_2", "head")
MESH = pl.DeviceIdType.MESH
HIGHEST = lax.Precision.HIGHEST
NEG = -1e30
UNIT = 256
HD = 128
SCALE = HD**-0.5
SCALE2 = SCALE * math.log2(math.e)
PLANE = 8
ZS = 8
XS = 4
PAIRS = ZS * XS
BF = jnp.bfloat16
F32 = jnp.float32


def dot(a, b, dims, precision=None):
    return lax.dot_general(a, b, (dims, ((), ())), precision=precision, preferred_element_type=F32)


def nn(a, b, precision=None):
    return dot(a, b, ((1,), (0,)), precision)


def nt(a, b):
    return dot(a, b, ((1,), (1,)))


def tn(a, b):
    return dot(a, b, ((0,), (0,)))


def kernel(
    k6, v6, q6, g6, xs, dy, st, rates, skips, bc, s0,
    dq6, dk6, dv6, gx, gst, gbc, gdec, gskip,
    kv, qg, stat, og, tscr, dscr,
    lb, sb, lrow, rrow, skr, whr, cbt, wsum, gb_acc, gc_acc, g0, ec,
    b_in, c_in, ldr, str_, car, plin, eplane, pplane, zt, zin, incout, inc,
    gbcl, gbin, tsrc, tpl, tz_src, tz,
    yin_s, yin_r, x1_s, x1_r, x2_s, x2_r, st_s, st_r, yo_s, yo_r,
    s1_s, s1_r, s2_s, s2_r, s3_s, s3_r, hb_s, hb_r, ta_s, ta_r, tb_s, tb_r,
):
    z, x, yh, hd = [lax.axis_index(a) for a in AXES]
    yl, core = hd // 2, hd % 2
    j = z * XS + x
    m = x * 2 + yh
    other = (1 - yl) * 2 + core
    heads = xs.shape[0]

    def at_pair(d):
        t = (j + d + PAIRS) % PAIRS
        return (t // XS, t % XS, yh, hd)

    def at_plane(mm):
        return (z, mm // 2, mm % 2, hd)

    def at_z(zz):
        return (zz, x, yh, hd)

    def at_head(hh):
        return (z, x, yh, hh)

    def at_y(k):
        return (z, x, k, other)

    def rcopy(src, dst, ss, rs, to):
        return pltpu.make_async_remote_copy(
            src_ref=src, dst_ref=dst, send_sem=ss, recv_sem=rs, device_id=to, device_id_type=MESH
        )

    peers = [at_y(0), at_y(1), at_pair(1), at_pair(-1), at_pair(2), at_pair(-2)]
    peers += [at_plane((m + o) % PLANE) for o in range(1, PLANE)]
    peers += [at_z((z + o) % ZS) for o in range(1, ZS)]
    peers += [at_head((hd + o) % 4) for o in range(1, 4)]
    barrier = pltpu.get_barrier_semaphore()
    for p in peers:
        pl.semaphore_signal(barrier, inc=1, device_id=p, device_id_type=MESH)
    pl.semaphore_wait(barrier, len(peers))

    sources = ((k6, v6), (q6, g6))
    lands = ((kv, 4), (qg, 0))

    def y_in(h, w, t, k, sender):
        buf, base = lands[w]
        return rcopy(
            sources[w][t].at[3 * k + h], buf.at[base + sender, h, t],
            yin_s.at[w, h, t, k], yin_r.at[w, h, t, sender], at_y(k),
        )

    def start_y_in(h):
        for w in range(2):
            for t in range(2):
                for k in range(2):
                    y_in(h, w, t, k, yh).start()

    def wait_y_in(h, w):
        for t in range(2):
            for k in range(2):
                y_in(h, w, t, k, k).wait_recv()

    def hop(n, w, h):
        if w == 0:
            src, dst, to = (kv.at[pl.ds(6 - 2 * n, 2), h], kv.at[pl.ds(4 - 2 * n, 2), h], at_pair(1))
        else:
            src, dst, to = (qg.at[pl.ds(2 * n - 2, 2), h], qg.at[pl.ds(2 * n, 2), h], at_pair(-1))
        ss, rs = ((x1_s, x1_r), (x2_s, x2_r))[n - 1]
        return rcopy(src, dst, ss.at[w, h], rs.at[w, h], to)

    def stat_copy(h, d):
        return rcopy(
            stat.at[pl.ds(0, 2), h], stat.at[pl.ds(2 * d, 2), h],
            st_s.at[d - 1, h], st_r.at[d - 1, h], at_pair(-d),
        )

    outs = (dq6, dk6, dv6)

    def y_out(n, h, i, sender):
        return rcopy(
            og.at[n, h, i], outs[n].at[3 * sender + h],
            yo_s.at[n, h, i], yo_r.at[n, h, sender], at_y(i),
        )

    def s1(o, to_m, from_m):
        return rcopy(
            car.at[to_m], plin.at[from_m],
            s1_s.at[o - 1], s1_r.at[o - 1], at_plane(to_m),
        )

    def s2(o, to_z, from_z):
        return rcopy(zt, zin.at[from_z], s2_s.at[o - 1], s2_r.at[o - 1], at_z(to_z))

    def s3(o, to_m, from_m):
        return rcopy(
            incout.at[to_m], inc.at[from_m],
            s3_s.at[o - 1], s3_r.at[o - 1], at_plane(to_m),
        )

    def hb(o, to_h, from_h):
        return rcopy(
            gbcl.at[pl.ds(pl.multiple_of(64 * to_h, 64), 64), :], gbin.at[from_h],
            hb_s.at[o - 1], hb_r.at[o - 1], at_head(to_h),
        )

    def ta(o, to_m, from_m):
        return rcopy(tsrc, tpl.at[from_m], ta_s.at[o - 1], ta_r.at[o - 1], at_plane(to_m))

    def tb(o, to_z, from_z):
        return rcopy(tz_src, tz.at[from_z], tb_s.at[o - 1], tb_r.at[o - 1], at_z(to_z))

    def start_all(make, mine, count):
        for o in range(1, count):
            make(o, (mine + o) % count, mine).start()

    def recv_all(make, mine, count):
        for o in range(1, count):
            make(o, mine, (mine + count - o) % count).wait_recv()

    def sent_all(make, mine, count):
        for o in range(1, count):
            make(o, (mine + o) % count, mine).wait_send()

    rowi = lax.broadcasted_iota(jnp.int32, (UNIT, UNIT), 0)
    coli = lax.broadcasted_iota(jnp.int32, (UNIT, UNIT), 1)

    start_y_in(0)
    b_in[...] = bc[:, :NSTATE]
    c_in[...] = bc[:, NSTATE:]
    ldr[...] = jnp.zeros_like(ldr)
    str_[...] = jnp.zeros_like(str_)
    str_[0:heads, :] = st[...]
    for h in range(heads):
        ldr[h : h + 1, :] = st[h : h + 1, :] * rates[h]
    lrow[...] = nn(ldr[...], (rowi <= coli).astype(F32), HIGHEST)
    lcol = lrow[...].T
    steps = str_[...].T
    decays = jnp.exp(lcol[UNIT - 1 : UNIT, :])
    sublane = lax.broadcasted_iota(jnp.int32, (8, HD), 0)

    def as_terms(row):
        high = row.astype(BF).astype(F32)
        middle = (row - high).astype(BF).astype(F32)
        low = row - high - middle
        terms = jnp.where(sublane == 0, high, jnp.where(sublane == 1, middle, low))
        return jnp.where(sublane < 3, terms, 0.0).astype(BF)

    def from_terms(tile):
        return jnp.sum(tile.astype(F32), axis=0, keepdims=True)

    for h in range(heads):
        lb[h] = jnp.broadcast_to(lcol[:, h : h + 1], (UNIT, HD))
        sb[h] = jnp.broadcast_to(steps[:, h : h + 1], (UNIT, HD))

    def summary(h, carry):
        scaled = (dy[h].astype(F32) * jnp.exp(lb[h])).astype(BF)
        part = tn(c_in[...], scaled)
        for i in range(PLANE):
            car[i, h] = part[8 * i : 8 * i + 8].astype(BF)
        return carry

    lax.fori_loop(0, heads, summary, 0)
    decay_terms = as_terms(decays)
    for i in range(PLANE):
        car[i, heads] = decay_terms
    start_all(s1, m, PLANE)
    start_y_in(1)
    start_y_in(2)
    plin[m] = car[m]

    cbt[...] = nt(b_in[...], c_in[...])

    def send_own(h):
        for w in range(2):
            wait_y_in(h, w)
            hop(1, w, h).start()

    def send_next(h):
        for w in range(2):
            hop(1, w, h).wait_recv()
            hop(2, w, h).start()

    send_own(0)

    recv_all(s1, m, PLANE)
    acc = [jnp.zeros((8, HD), F32)] * heads
    prod = [jnp.ones((8, HD), F32)] * heads
    row_prod = jnp.ones((1, HD), F32)
    for mm in reversed(range(PLANE)):
        row = from_terms(plin[mm, heads])
        row_prod = row_prod * row
        for h in range(heads):
            eplane[mm, h] = acc[h]
            pplane[mm, h] = prod[h]
            decay = jnp.broadcast_to(row[:, h : h + 1], (8, HD))
            acc[h] = plin[mm, h].astype(F32) + decay * acc[h]
            prod[h] = prod[h] * decay
    for h in range(heads):
        zt[h] = acc[h].astype(BF)
    zt[heads] = as_terms(row_prod)
    start_all(s2, z, ZS)
    zin[z] = zt[...]

    send_own(1)
    recv_all(s2, z, ZS)
    acc = [jnp.zeros((8, HD), F32)] * heads
    for zz in reversed(range(1, ZS)):
        row = from_terms(zin[zz, heads])
        for h in range(heads):
            decay = jnp.broadcast_to(row[:, h : h + 1], (8, HD))
            acc[h] = jnp.where(zz > z, zin[zz, h].astype(F32) + decay * acc[h], acc[h])
    for mm in range(PLANE):
        for h in range(heads):
            incout[mm, h] = (eplane[mm, h] + pplane[mm, h] * acc[h]).astype(BF)
    start_all(s3, m, PLANE)
    inc[m] = incout[m]

    send_next(0)
    send_own(2)
    send_next(1)

    for ref in (rrow, skr, whr, wsum, gb_acc, gc_acc, g0, ec, tsrc):
        ref[...] = jnp.zeros_like(ref)
    lanes = lax.broadcasted_iota(jnp.int32, (UNIT, HD), 1)

    def wide(t):
        return jnp.concatenate([t, t], axis=1)

    def grads(h, carry):
        b_rows, c_rows = (b_in[...], c_in[...])
        lc, sc = (lb[h], sb[h])
        lr = lrow[pl.ds(h, 1), :]
        x_h, dy_h = (xs[h], dy[h])
        cb = cbt[...]
        decay = jnp.exp(jnp.where(coli >= rowi, lr - wide(lc), NEG))
        crossed = decay * nt(x_h, dy_h)
        weighted = crossed * wide(sc)
        wsum[...] += weighted
        rrow[pl.ds(h, 1), :] = jnp.sum(weighted * cb, axis=0, keepdims=True)
        paired = crossed * cb
        mixing = (decay * cb).astype(BF)
        tail = jnp.exp(lc[UNIT - 1 : UNIT, :] - lc)
        weights = jnp.exp(lc)
        inc_f = jnp.concatenate([inc[i, h].astype(F32) for i in range(PLANE)], axis=0)
        s0_f = s0[h]
        inc_h, s0_h = (inc_f.astype(BF), s0_f.astype(BF))
        dy_f = dy_h.astype(F32)
        driven_grad = nn(mixing, dy_h) + tail * nn(b_rows, inc_h)
        gx[h] = (sc * driven_grad + skips[h] * dy_f).astype(BF)
        late = nt(x_h, inc_h) * tail[:, :NSTATE]
        gb_acc[...] += sc[:, :NSTATE] * late
        early = nt(dy_h, s0_h) * weights[:, :NSTATE]
        gc_acc[...] += early
        own = jnp.sum(paired[:, :HD] + paired[:, HD:], axis=1, keepdims=True)
        own = own + jnp.sum(late * b_rows.astype(F32), axis=1, keepdims=True)
        first = jnp.sum(early * c_rows.astype(F32), axis=1, keepdims=True)
        here = lanes == h
        g0[...] += jnp.where(here, own, 0.0)
        ec[...] += jnp.where(here, first, 0.0)
        skr[pl.ds(h, 1), :] = jnp.sum(dy_f * x_h.astype(F32), axis=0, keepdims=True)
        whr[pl.ds(h, 1), :] = jnp.sum(inc_f * s0_f, axis=0, keepdims=True)
        return carry

    def window(h):
        def block(i, carry):
            q, g = (qg[i, h, 0], qg[i, h, 1])
            top = None
            for u in range(5):
                s = nt(kv[i + u, h, 0], q) * SCALE2
                if u == 0:
                    s = jnp.where(rowi > coli, s, NEG)
                if u == 4:
                    s = jnp.where(rowi <= coli, s, NEG)
                else:
                    s = s + jnp.where(2 * j + i + u >= 4, 0.0, NEG)
                tscr[u] = s
                best = jnp.max(s, axis=0, keepdims=True)
                top = best if top is None else jnp.maximum(top, best)
            total = jnp.zeros((1, UNIT), F32)
            delta = jnp.zeros((1, UNIT), F32)
            for u in range(5):
                e = jnp.exp2(tscr[u] - top)
                dp = nt(kv[i + u, h, 1], g)
                total = total + jnp.sum(e, axis=0, keepdims=True)
                delta = delta + jnp.sum(e * dp, axis=0, keepdims=True)
                tscr[u] = e
                dscr[u] = dp
            inverse = 1.0 / total
            delta = delta * inverse
            out = jnp.zeros((HD, UNIT), F32)
            for u in range(5):
                ds = (tscr[u] * (dscr[u] - delta)).astype(BF)
                out = out + tn(kv[i + u, h, 0], ds)
            og[0, h, i] = (out * (inverse * SCALE)).T.astype(BF)
            stat[i, h, 0:1, :] = top + jnp.log2(total)
            stat[i, h, 1:2, :] = delta
            return carry

        lax.fori_loop(0, 2, block, 0)

    def key_pass(h):
        def block(i, carry):
            k, v = (kv[4 + i, h, 0], kv[4 + i, h, 1])
            dk = jnp.zeros((UNIT, HD), F32)
            dv = jnp.zeros((UNIT, HD), F32)
            for u in range(5):
                q, g = (qg[i + u, h, 0], qg[i + u, h, 1])
                s = nt(k, q) * SCALE2 - stat[i + u, h, 0:1, :]
                if u == 0:
                    s = jnp.where(coli >= rowi, s, NEG)
                else:
                    s = s + jnp.where(2 * j + i + u < 2 * PAIRS, 0.0, NEG)
                if u == 4:
                    s = jnp.where(coli < rowi, s, NEG)
                p = jnp.exp2(s)
                dv = dv + nn(p.astype(BF), g)
                ds = (p * (nt(v, g) - stat[i + u, h, 1:2, :])).astype(BF)
                dk = dk + nn(ds, q)
            og[1, h, i] = (dk * SCALE).astype(BF)
            og[2, h, i] = dv.astype(BF)
            return carry

        lax.fori_loop(0, 2, block, 0)

    def windows(h):
        hop(2, 0, h).wait_recv()
        window(h)
        for d in (1, 2):
            stat_copy(h, d).start()
        for i in range(2):
            y_out(0, h, i, yh).start()

    def keys(h):
        hop(2, 1, h).wait_recv()
        for d in (1, 2):
            stat_copy(h, d).wait_recv()
        key_pass(h)
        for n in (1, 2):
            for i in range(2):
                y_out(n, h, i, yh).start()

    for h in range(3):
        stat[0:2, h] = jnp.zeros((2, 8, UNIT), F32)
    windows(0)

    recv_all(s3, m, PLANE)
    lax.fori_loop(0, heads // 2, grads, 0)
    send_next(2)
    lax.fori_loop(heads // 2, heads, grads, 0)
    w_all = wsum[...]
    gb_all = gb_acc[...] + nn(w_all, c_in[...].astype(F32), HIGHEST)
    gc_all = gc_acc[...] + nn(w_all.T, b_in[...].astype(F32), HIGHEST)
    gbcl[...] = jnp.concatenate([gb_all, gc_all], axis=1)
    start_all(hb, hd, 4)
    gbin[hd] = gbcl[pl.ds(pl.multiple_of(64 * hd, 64), 64), :]
    early_all = ec[...]
    change = steps * g0[...] - rrow[...].T - early_all
    strict = (coli < rowi).astype(F32)
    whole = decays * jnp.sum(whr[...].T, axis=0, keepdims=True)
    grad_log = nn(strict, change, HIGHEST) + (jnp.sum(early_all, axis=0, keepdims=True) + whole)
    own_rows, log_rows = (g0[...].T, grad_log.T)
    for h in range(heads):
        gst[h : h + 1, :] = own_rows[h : h + 1, :] + rates[h] * log_rows[h : h + 1, :]
    tsrc[0:1, :] = jnp.sum(steps * grad_log, axis=0, keepdims=True)
    tsrc[1:2, :] = jnp.sum(skr[...].T, axis=0, keepdims=True)
    start_all(ta, m, PLANE)
    tpl[m] = tsrc[...]

    windows(1)
    keys(0)

    recv_all(ta, m, PLANE)
    plane_sum = tpl[0]
    for mm in range(1, PLANE):
        plane_sum = plane_sum + tpl[mm]
    tz_src[...] = plane_sum
    start_all(tb, z, ZS)
    tz[z] = plane_sum

    keys(1)
    windows(2)

    recv_all(hb, hd, 4)
    gbc[...] = ((gbin[0] + gbin[1]) + gbin[2]) + gbin[3]
    recv_all(tb, z, ZS)
    total = tz[0]
    for zz in range(1, ZS):
        total = total + tz[zz]
    gdec[...] = total[0:1, :heads]
    gskip[...] = total[1:2, :heads]

    keys(2)

    for h in range(3):
        for n in range(3):
            for i in range(2):
                y_out(n, h, i, i).wait_recv()
    for h in range(3):
        for w in range(2):
            for t in range(2):
                for k in range(2):
                    y_in(h, w, t, k, yh).wait_send()
            for n in (1, 2):
                hop(n, w, h).wait_send()
        for d in (1, 2):
            stat_copy(h, d).wait_send()
        for n in range(3):
            for i in range(2):
                y_out(n, h, i, yh).wait_send()
    sent_all(s1, m, PLANE)
    sent_all(s2, z, ZS)
    sent_all(s3, m, PLANE)
    sent_all(hb, hd, 4)
    sent_all(ta, m, PLANE)
    sent_all(tb, z, ZS)


def finish_kernel(*refs):
    count = len(refs) // 2
    sems = refs[-1]
    copies = [
        pltpu.make_async_copy(refs[n], refs[count + n], sems.at[n]) for n in range(count)
    ]
    for copy in copies:
        copy.start()
    for copy in copies:
        copy.wait()


def finish(arrays):
    count = len(arrays)
    return pl.pallas_call(
        finish_kernel,
        name="finish",
        out_shape=[jax.ShapeDtypeStruct(a.shape, a.dtype) for a in arrays],
        in_specs=[pl.BlockSpec(memory_space=pltpu.VMEM)] * count,
        out_specs=[pl.BlockSpec(memory_space=pl.ANY)] * count,
        scratch_shapes=[pltpu.SemaphoreType.DMA((count,))],
    )(*[pltpu.with_memory_space_constraint(a, pltpu.VMEM) for a in arrays])


def shards(
    queries, key_vectors, values, out_grad, ssm_input, ssm_out_grad,
    step_sizes, decay_rates, skip_gains, bc_rows, saved_states,
):
    heads = ssm_input.shape[1]
    by_head = [
        jnp.transpose(t, (1, 0, 2))
        for t in (key_vectors, values, queries, out_grad, ssm_input, ssm_out_grad)
    ]
    vmem = pl.BlockSpec(memory_space=pltpu.VMEM)
    smem = pl.BlockSpec(memory_space=pltpu.SMEM)

    def kept(s, t=F32):
        return pltpu.VMEM(s, t)

    def scratch(s, t=F32):
        return pltpu.VMEM(s, t)

    dma = pltpu.SemaphoreType.DMA
    wide = (heads, UNIT, HD)
    tile = (8, HD)
    out = pl.pallas_call(
        kernel,
        name="mixers",
        out_shape=[
            kept((6, UNIT, HD), BF), kept((6, UNIT, HD), BF), kept((6, UNIT, HD), BF),
            kept(wide, BF), kept((heads, UNIT)), kept((UNIT // 4, HD)),
            kept((1, heads)), kept((1, heads)),
        ],
        in_specs=[vmem] * 7 + [smem] * 2 + [vmem] * 2,
        out_specs=[vmem] * 8,
        scratch_shapes=[
            scratch((6, 3, 2, UNIT, HD), BF), scratch((6, 3, 2, UNIT, HD), BF),
            scratch((6, 3, 8, UNIT)), scratch((3, 3, 2, UNIT, HD), BF),
            scratch((5, UNIT, UNIT)), scratch((5, UNIT, UNIT)),
            scratch(wide), scratch(wide), scratch((HD, UNIT)), scratch((HD, UNIT)),
            scratch((HD, HD)), scratch((HD, HD)), scratch((UNIT, UNIT)), scratch((UNIT, UNIT)),
            scratch((UNIT, NSTATE)), scratch((UNIT, NSTATE)), scratch((UNIT, HD)), scratch((UNIT, HD)),
            scratch((UNIT, NSTATE), BF), scratch((UNIT, NSTATE), BF), scratch((HD, UNIT)), scratch((HD, UNIT)),
            scratch((PLANE, heads + 1, *tile), BF), scratch((PLANE, heads + 1, *tile), BF),
            scratch((PLANE, heads, *tile)), scratch((PLANE, heads, *tile)),
            scratch((heads + 1, *tile), BF), scratch((ZS, heads + 1, *tile), BF),
            scratch((PLANE, heads, *tile), BF), scratch((PLANE, heads, *tile), BF),
            scratch((UNIT, HD)), scratch((4, UNIT // 4, HD)),
            scratch(tile), scratch((PLANE, *tile)), scratch(tile), scratch((ZS, *tile)),
            dma((2, 3, 2, 2)), dma((2, 3, 2, 2)), dma((2, 3)), dma((2, 3)), dma((2, 3)), dma((2, 3)),
            dma((2, 3)), dma((2, 3)), dma((3, 3, 2)), dma((3, 3, 2)),
            dma((7,)), dma((7,)), dma((7,)), dma((7,)), dma((7,)), dma((7,)),
            dma((3,)), dma((3,)), dma((7,)), dma((7,)), dma((7,)), dma((7,)),
        ],
        compiler_params=pltpu.CompilerParams(
            collective_id=0, has_side_effects=True, vmem_limit_bytes=60 * 1024 * 1024
        ),
    )(
        *by_head, step_sizes.T, decay_rates, skip_gains, bc_rows, saved_states[0]
    )
    dq6, dk6, dv6, gx, gst, gbc, gdec, gskip = finish(out)
    return (
        jnp.transpose(dq6, (1, 0, 2)),
        jnp.transpose(dk6, (1, 0, 2)),
        jnp.transpose(dv6, (1, 0, 2)),
        jnp.transpose(gx, (1, 0, 2)),
        gst.T,
        gbc,
        gdec[0],
        gskip[0],
    )


def solution(mesh):
    torus = Mesh(mesh.devices.reshape(ZS, XS, 2, mesh.shape["head"]), AXES)
    token_head = P(SEQ, "head", None)
    in_specs = (token_head,) * 6 + (
        P(SEQ, "head"), P("head"), P("head"), P(SEQ, None), P(SEQ, "head", None, None),
    )
    out_specs = (token_head,) * 4 + (P(SEQ, "head"), P(SEQ_HEAD, None), P("head"), P("head"))
    return jax.shard_map(shards, mesh=torus, in_specs=in_specs, out_specs=out_specs, check_vma=False)
```

```python
import functools
import math

import jax
import jax.numpy as jnp
from jax import lax
from jax.experimental import pallas as pl
from jax.experimental.pallas import tpu as pltpu
from jax.sharding import Mesh
from jax.sharding import PartitionSpec as P

NSTATE = 64
SEQ = ("seq_0", "seq_1", "seq_2")
SEQ_HEAD = ("seq_0", "seq_1", "seq_2", "head")
AXES = ("seq_0", "seq_1", "seq_2", "head")
MESH = pl.DeviceIdType.MESH
HIGHEST = lax.Precision.HIGHEST
NEG = -1e30
UNIT = 256
HD = 128
SCALE = HD**-0.5
SCALE2 = SCALE * math.log2(math.e)
PLANE = 8
ZS = 8
XS = 4
PAIRS = ZS * XS
BF = jnp.bfloat16
F32 = jnp.float32


def dot(a, b, dims, precision=None):
    return lax.dot_general(a, b, (dims, ((), ())), precision=precision, preferred_element_type=F32)


def nn(a, b, precision=None):
    return dot(a, b, ((1,), (0,)), precision)


def nt(a, b):
    return dot(a, b, ((1,), (1,)))


def tn(a, b):
    return dot(a, b, ((0,), (0,)))


def kernel(
    k6_in, v6_in, q6_in, g6_in, xs_in, dy_in, st_in, rates, skips, bc_in, s0_in,
    dq6, dk6, dv6, gx, gst, gbc, gdec, gskip,
    k6, v6, q6, g6, xs, dy, st, bc, s0, load_sem,
    kv, qg, stat, og, tscr, dscr,
    lb, sb, lrow, rrow, skr, whr, cbt, wsum, gb_acc, gc_acc, g0, ec,
    gdr, b_in, c_in, ldr, str_, car, plin, eplane, pplane, zt, zin, incout, inc,
    gbcl, gbin, tsrc, tpl, tz_src, tz,
    yin_s, yin_r, x1_s, x1_r, x2_s, x2_r, st_s, st_r, yo_s, yo_r,
    s1_s, s1_r, s2_s, s2_r, s3_s, s3_r, hb_s, hb_r, ta_s, ta_r, tb_s, tb_r,
):
    z, x, yh, hd = [lax.axis_index(a) for a in AXES]
    yl, core = hd // 2, hd % 2
    j = z * XS + x
    m = x * 2 + yh
    other = (1 - yl) * 2 + core
    heads = xs_in.shape[0]

    def at_pair(d):
        t = (j + d + PAIRS) % PAIRS
        return (t // XS, t % XS, yh, hd)

    def at_plane(mm):
        return (z, mm // 2, mm % 2, hd)

    def at_z(zz):
        return (zz, x, yh, hd)

    def at_head(hh):
        return (z, x, yh, hh)

    def at_y(k):
        return (z, x, k, other)

    def rcopy(src, dst, ss, rs, to):
        return pltpu.make_async_remote_copy(
            src_ref=src, dst_ref=dst, send_sem=ss, recv_sem=rs, device_id=to, device_id_type=MESH
        )

    peers = [at_y(0), at_y(1), at_pair(1), at_pair(-1), at_pair(2), at_pair(-2)]
    peers += [at_plane((m + o) % PLANE) for o in range(1, PLANE)]
    peers += [at_z((z + o) % ZS) for o in range(1, ZS)]
    peers += [at_head((hd + o) % 4) for o in range(1, 4)]
    loads = [
        pltpu.make_async_copy(src, dst, load_sem.at[n])
        for n, (src, dst) in enumerate(
            (
                (k6_in, k6), (v6_in, v6), (q6_in, q6), (g6_in, g6), (st_in, st),
                (bc_in, bc), (dy_in, dy), (xs_in, xs), (s0_in, s0),
            )
        )
    ]
    for load in loads:
        load.start()
    barrier = pltpu.get_barrier_semaphore()
    for p in peers:
        pl.semaphore_signal(barrier, inc=1, device_id=p, device_id_type=MESH)
    pl.semaphore_wait(barrier, len(peers))

    sources = ((k6, v6), (q6, g6))
    lands = ((kv, 4), (qg, 0))

    def y_in(h, w, t, k, sender):
        buf, base = lands[w]
        return rcopy(
            sources[w][t].at[3 * k + h], buf.at[base + sender, h, t],
            yin_s.at[w, h, t, k], yin_r.at[w, h, t, sender], at_y(k),
        )

    def start_y_in(h):
        for w in range(2):
            for t in range(2):
                for k in range(2):
                    y_in(h, w, t, k, yh).start()

    def wait_y_in(h, w):
        for t in range(2):
            for k in range(2):
                y_in(h, w, t, k, k).wait_recv()

    def hop(n, w, h):
        if w == 0:
            src, dst, to = (kv.at[pl.ds(6 - 2 * n, 2), h], kv.at[pl.ds(4 - 2 * n, 2), h], at_pair(1))
        else:
            src, dst, to = (qg.at[pl.ds(2 * n - 2, 2), h], qg.at[pl.ds(2 * n, 2), h], at_pair(-1))
        ss, rs = ((x1_s, x1_r), (x2_s, x2_r))[n - 1]
        return rcopy(src, dst, ss.at[w, h], rs.at[w, h], to)

    def stat_copy(h, d):
        return rcopy(
            stat.at[pl.ds(0, 2), h], stat.at[pl.ds(2 * d, 2), h],
            st_s.at[d - 1, h], st_r.at[d - 1, h], at_pair(-d),
        )

    outs = (dq6, dk6, dv6)

    def y_out(n, h, i, sender):
        return rcopy(
            og.at[n, h, i], outs[n].at[3 * sender + h],
            yo_s.at[n, h, i], yo_r.at[n, h, sender], at_y(i),
        )

    def s1(o, to_m, from_m):
        return rcopy(
            car.at[to_m], plin.at[from_m],
            s1_s.at[o - 1], s1_r.at[o - 1], at_plane(to_m),
        )

    def s2(o, to_z, from_z):
        return rcopy(zt, zin.at[from_z], s2_s.at[o - 1], s2_r.at[o - 1], at_z(to_z))

    def s3(o, to_m, from_m):
        return rcopy(
            incout.at[to_m], inc.at[from_m],
            s3_s.at[o - 1], s3_r.at[o - 1], at_plane(to_m),
        )

    def hb(o, to_h, from_h):
        return rcopy(
            gbcl.at[pl.ds(pl.multiple_of(64 * to_h, 64), 64), :], gbin.at[from_h],
            hb_s.at[o - 1], hb_r.at[o - 1], at_head(to_h),
        )

    def ta(o, to_m, from_m):
        return rcopy(tsrc, tpl.at[from_m], ta_s.at[o - 1], ta_r.at[o - 1], at_plane(to_m))

    def tb(o, to_z, from_z):
        return rcopy(tz_src, tz.at[from_z], tb_s.at[o - 1], tb_r.at[o - 1], at_z(to_z))

    def start_all(make, mine, count):
        for o in range(1, count):
            make(o, (mine + o) % count, mine).start()

    def recv_all(make, mine, count):
        for o in range(1, count):
            make(o, mine, (mine + count - o) % count).wait_recv()

    def sent_all(make, mine, count):
        for o in range(1, count):
            make(o, (mine + o) % count, mine).wait_send()

    rowi = lax.broadcasted_iota(jnp.int32, (UNIT, UNIT), 0)
    coli = lax.broadcasted_iota(jnp.int32, (UNIT, UNIT), 1)

    for load in loads[:4]:
        load.wait()
    start_y_in(0)
    for load in loads[4:]:
        load.wait()
    b_in[...] = bc[:, :NSTATE]
    c_in[...] = bc[:, NSTATE:]
    ldr[...] = jnp.zeros_like(ldr)
    str_[...] = jnp.zeros_like(str_)
    str_[0:heads, :] = st[...]
    for h in range(heads):
        ldr[h : h + 1, :] = st[h : h + 1, :] * rates[h]
    lrow[...] = nn(ldr[...], (rowi <= coli).astype(F32), HIGHEST)
    lcol = lrow[...].T
    steps = str_[...].T
    decays = jnp.exp(lcol[UNIT - 1 : UNIT, :])
    sublane = lax.broadcasted_iota(jnp.int32, (8, HD), 0)

    def as_terms(row):
        high = row.astype(BF).astype(F32)
        middle = (row - high).astype(BF).astype(F32)
        low = row - high - middle
        terms = jnp.where(sublane == 0, high, jnp.where(sublane == 1, middle, low))
        return jnp.where(sublane < 3, terms, 0.0).astype(BF)

    def from_terms(tile):
        return jnp.sum(tile.astype(F32), axis=0, keepdims=True)

    for h in range(heads):
        lb[h] = jnp.broadcast_to(lcol[:, h : h + 1], (UNIT, HD))
        sb[h] = jnp.broadcast_to(steps[:, h : h + 1], (UNIT, HD))

    def summary_of(h):
        scaled = (dy[h].astype(F32) * jnp.exp(lb[h])).astype(BF)
        part = tn(c_in[...], scaled)
        for i in range(PLANE):
            car[i, h] = part[8 * i : 8 * i + 8].astype(BF)

    def summary(n, carry):
        for i in range(3):
            summary_of(3 * n + i)
        return carry

    lax.fori_loop(0, heads // 3, summary, 0)
    decay_terms = as_terms(decays)
    for i in range(PLANE):
        car[i, heads] = decay_terms
    start_all(s1, m, PLANE)
    start_y_in(1)
    start_y_in(2)
    plin[m] = car[m]

    cbt[...] = nt(b_in[...], c_in[...])

    def send_own(h):
        for w in range(2):
            wait_y_in(h, w)
            hop(1, w, h).start()

    def send_next(h):
        for w in range(2):
            hop(1, w, h).wait_recv()
            hop(2, w, h).start()

    for ref in (rrow, skr, whr, wsum, gb_acc, gc_acc, g0, ec, tsrc):
        ref[...] = jnp.zeros_like(ref)
    lanes = lax.broadcasted_iota(jnp.int32, (UNIT, HD), 1)

    def wide(t):
        return jnp.concatenate([t, t], axis=1)

    def grads(h, carry):
        c_rows = c_in[...]
        lc, sc = (lb[h], sb[h])
        lr = lrow[pl.ds(h, 1), :]
        x_h, dy_h = (xs[h], dy[h])
        cb = cbt[...]
        decay = jnp.exp(jnp.where(coli >= rowi, lr - wide(lc), NEG))
        crossed = decay * nt(x_h, dy_h)
        weighted = crossed * wide(sc)
        wsum[...] += weighted
        rrow[pl.ds(h, 1), :] = jnp.sum(weighted * cb, axis=0, keepdims=True)
        paired = crossed * cb
        gdr[h] = nn((decay * cb).astype(BF), dy_h)
        early = nt(dy_h, s0[h].astype(BF)) * jnp.exp(lc)[:, :NSTATE]
        gc_acc[...] += early
        own = jnp.sum(paired[:, :HD] + paired[:, HD:], axis=1, keepdims=True)
        first = jnp.sum(early * c_rows.astype(F32), axis=1, keepdims=True)
        here = lanes == h
        g0[...] += jnp.where(here, own, 0.0)
        ec[...] += jnp.where(here, first, 0.0)
        skr[pl.ds(h, 1), :] = jnp.sum(dy_h.astype(F32) * x_h.astype(F32), axis=0, keepdims=True)
        return carry

    def carried_of(h):
        b_rows = b_in[...]
        lc, sc = (lb[h], sb[h])
        tail = jnp.exp(lc[UNIT - 1 : UNIT, :] - lc)
        inc_f = jnp.concatenate([inc[i, h].astype(F32) for i in range(PLANE)], axis=0)
        inc_h = inc_f.astype(BF)
        driven_grad = gdr[h] + tail * nn(b_rows, inc_h)
        gx[h] = (sc * driven_grad + skips[h] * dy[h].astype(F32)).astype(BF)
        late = nt(xs[h], inc_h) * tail[:, :NSTATE]
        gb_acc[...] += sc[:, :NSTATE] * late
        own = jnp.sum(late * b_rows.astype(F32), axis=1, keepdims=True)
        g0[...] += jnp.where(lanes == h, own, 0.0)
        whr[pl.ds(h, 1), :] = jnp.sum(inc_f * s0[h], axis=0, keepdims=True)

    def carried(n, carry):
        for i in range(2):
            carried_of(2 * n + i)
        return carry

    send_own(0)

    recv_all(s1, m, PLANE)
    acc = [jnp.zeros((8, HD), F32)] * heads
    prod = [jnp.ones((8, HD), F32)] * heads
    row_prod = jnp.ones((1, HD), F32)
    for mm in reversed(range(PLANE)):
        row = from_terms(plin[mm, heads])
        row_prod = row_prod * row
        for h in range(heads):
            eplane[mm, h] = acc[h]
            pplane[mm, h] = prod[h]
            decay = jnp.broadcast_to(row[:, h : h + 1], (8, HD))
            acc[h] = plin[mm, h].astype(F32) + decay * acc[h]
            prod[h] = prod[h] * decay
    for h in range(heads):
        zt[h] = acc[h].astype(BF)
    zt[heads] = as_terms(row_prod)
    start_all(s2, z, ZS)
    zin[z] = zt[...]

    send_own(1)
    send_next(0)
    send_own(2)
    lax.fori_loop(0, heads // 2, grads, 0)
    recv_all(s2, z, ZS)
    acc = [jnp.zeros((8, HD), F32)] * heads
    for zz in reversed(range(1, ZS)):
        row = from_terms(zin[zz, heads])
        for h in range(heads):
            decay = jnp.broadcast_to(row[:, h : h + 1], (8, HD))
            acc[h] = jnp.where(zz > z, zin[zz, h].astype(F32) + decay * acc[h], acc[h])
    for mm in range(PLANE):
        for h in range(heads):
            incout[mm, h] = (eplane[mm, h] + pplane[mm, h] * acc[h]).astype(BF)
    start_all(s3, m, PLANE)
    inc[m] = incout[m]

    send_next(1)
    lax.fori_loop(heads // 2, heads, grads, 0)

    def window(h):
        def block(i, carry):
            q, g = (qg[i, h, 0], qg[i, h, 1])
            top = None
            for u in range(5):
                s = nt(kv[i + u, h, 0], q) * SCALE2
                if u == 0:
                    s = jnp.where(rowi > coli, s, NEG)
                if u == 4:
                    s = jnp.where(rowi <= coli, s, NEG)
                else:
                    s = s + jnp.where(2 * j + i + u >= 4, 0.0, NEG)
                tscr[u] = s
                best = jnp.max(s, axis=0, keepdims=True)
                top = best if top is None else jnp.maximum(top, best)
            total = jnp.zeros((1, UNIT), F32)
            delta = jnp.zeros((1, UNIT), F32)
            for u in range(5):
                e = jnp.exp2(tscr[u] - top)
                dp = nt(kv[i + u, h, 1], g)
                total = total + jnp.sum(e, axis=0, keepdims=True)
                delta = delta + jnp.sum(e * dp, axis=0, keepdims=True)
                tscr[u] = e
                dscr[u] = dp
            inverse = 1.0 / total
            delta = delta * inverse
            out = jnp.zeros((HD, UNIT), F32)
            for u in range(5):
                ds = (tscr[u] * (dscr[u] - delta)).astype(BF)
                out = out + tn(kv[i + u, h, 0], ds)
            og[0, h, i] = (out * (inverse * SCALE)).T.astype(BF)
            stat[i, h, 0:1, :] = top + jnp.log2(total)
            stat[i, h, 1:2, :] = delta
            return carry

        lax.fori_loop(0, 2, block, 0)

    def key_pass(h):
        def block(i, carry):
            k, v = (kv[4 + i, h, 0], kv[4 + i, h, 1])
            dk = jnp.zeros((UNIT, HD), F32)
            dv = jnp.zeros((UNIT, HD), F32)
            for u in range(5):
                q, g = (qg[i + u, h, 0], qg[i + u, h, 1])
                s = nt(k, q) * SCALE2 - stat[i + u, h, 0:1, :]
                if u == 0:
                    s = jnp.where(coli >= rowi, s, NEG)
                else:
                    s = s + jnp.where(2 * j + i + u < 2 * PAIRS, 0.0, NEG)
                if u == 4:
                    s = jnp.where(coli < rowi, s, NEG)
                p = jnp.exp2(s)
                dv = dv + nn(p.astype(BF), g)
                ds = (p * (nt(v, g) - stat[i + u, h, 1:2, :])).astype(BF)
                dk = dk + nn(ds, q)
            og[1, h, i] = (dk * SCALE).astype(BF)
            og[2, h, i] = dv.astype(BF)
            return carry

        lax.fori_loop(0, 2, block, 0)

    def windows(h):
        hop(2, 0, h).wait_recv()
        window(h)
        for d in (1, 2):
            stat_copy(h, d).start()
        for i in range(2):
            y_out(0, h, i, yh).start()

    def keys(h):
        hop(2, 1, h).wait_recv()
        for d in (1, 2):
            stat_copy(h, d).wait_recv()
        key_pass(h)
        for n in (1, 2):
            for i in range(2):
                y_out(n, h, i, yh).start()

    for h in range(3):
        stat[0:2, h] = jnp.zeros((2, 8, UNIT), F32)
    windows(0)
    send_next(2)
    windows(1)
    keys(0)
    windows(2)
    keys(1)

    recv_all(s3, m, PLANE)
    lax.fori_loop(0, heads // 2, carried, 0)
    w_all = wsum[...]
    gb_all = gb_acc[...] + nn(w_all, c_in[...].astype(F32), HIGHEST)
    gc_all = gc_acc[...] + nn(w_all.T, b_in[...].astype(F32), HIGHEST)
    gbcl[...] = jnp.concatenate([gb_all, gc_all], axis=1)
    start_all(hb, hd, 4)
    gbin[hd] = gbcl[pl.ds(pl.multiple_of(64 * hd, 64), 64), :]
    early_all = ec[...]
    change = steps * g0[...] - rrow[...].T - early_all
    strict = (coli < rowi).astype(F32)
    whole = decays * jnp.sum(whr[...].T, axis=0, keepdims=True)
    grad_log = nn(strict, change, HIGHEST) + (jnp.sum(early_all, axis=0, keepdims=True) + whole)
    own_rows, log_rows = (g0[...].T, grad_log.T)
    for h in range(heads):
        gst[h : h + 1, :] = own_rows[h : h + 1, :] + rates[h] * log_rows[h : h + 1, :]
    tsrc[0:1, :] = jnp.sum(steps * grad_log, axis=0, keepdims=True)
    tsrc[1:2, :] = jnp.sum(skr[...].T, axis=0, keepdims=True)
    start_all(ta, m, PLANE)
    tpl[m] = tsrc[...]

    keys(2)

    recv_all(ta, m, PLANE)
    plane_sum = tpl[0]
    for mm in range(1, PLANE):
        plane_sum = plane_sum + tpl[mm]
    tz_src[...] = plane_sum
    start_all(tb, z, ZS)
    tz[z] = plane_sum
    recv_all(hb, hd, 4)
    gbc[...] = ((gbin[0] + gbin[1]) + gbin[2]) + gbin[3]
    recv_all(tb, z, ZS)
    total = tz[0]
    for zz in range(1, ZS):
        total = total + tz[zz]
    gdec[...] = total[0:1, :heads]
    gskip[...] = total[1:2, :heads]

    for h in range(3):
        for n in range(3):
            for i in range(2):
                y_out(n, h, i, i).wait_recv()
    for h in range(3):
        for w in range(2):
            for t in range(2):
                for k in range(2):
                    y_in(h, w, t, k, yh).wait_send()
            for n in (1, 2):
                hop(n, w, h).wait_send()
        for d in (1, 2):
            stat_copy(h, d).wait_send()
        for n in range(3):
            for i in range(2):
                y_out(n, h, i, yh).wait_send()
    sent_all(s1, m, PLANE)
    sent_all(s2, z, ZS)
    sent_all(s3, m, PLANE)
    sent_all(hb, hd, 4)
    sent_all(ta, m, PLANE)
    sent_all(tb, z, ZS)


def finish_kernel(*refs):
    count = len(refs) // 2
    sems = refs[-1]
    copies = [
        pltpu.make_async_copy(refs[n], refs[count + n], sems.at[n]) for n in range(count)
    ]
    for copy in copies:
        copy.start()
    for copy in copies:
        copy.wait()


def finish(arrays):
    count = len(arrays)
    return pl.pallas_call(
        finish_kernel,
        name="finish",
        out_shape=[jax.ShapeDtypeStruct(a.shape, a.dtype) for a in arrays],
        in_specs=[pl.BlockSpec(memory_space=pltpu.VMEM)] * count,
        out_specs=[pl.BlockSpec(memory_space=pl.ANY)] * count,
        scratch_shapes=[pltpu.SemaphoreType.DMA((count,))],
    )(*[pltpu.with_memory_space_constraint(a, pltpu.VMEM) for a in arrays])


def shards(
    queries, key_vectors, values, out_grad, ssm_input, ssm_out_grad,
    step_sizes, decay_rates, skip_gains, bc_rows, saved_states,
):
    heads = ssm_input.shape[1]
    by_head = [
        jnp.transpose(t, (1, 0, 2))
        for t in (key_vectors, values, queries, out_grad, ssm_input, ssm_out_grad)
    ]
    vmem = pl.BlockSpec(memory_space=pltpu.VMEM)
    hbm = pl.BlockSpec(memory_space=pl.ANY)
    smem = pl.BlockSpec(memory_space=pltpu.SMEM)

    def kept(s, t=F32):
        return pltpu.VMEM(s, t)

    def scratch(s, t=F32):
        return pltpu.VMEM(s, t)

    dma = pltpu.SemaphoreType.DMA
    wide = (heads, UNIT, HD)
    tile = (8, HD)
    out = pl.pallas_call(
        kernel,
        name="mixers",
        out_shape=[
            kept((6, UNIT, HD), BF), kept((6, UNIT, HD), BF), kept((6, UNIT, HD), BF),
            kept(wide, BF), kept((heads, UNIT)), kept((UNIT // 4, HD)),
            kept((1, heads)), kept((1, heads)),
        ],
        in_specs=[hbm] * 7 + [smem] * 2 + [hbm] * 2,
        out_specs=[vmem] * 8,
        scratch_shapes=[
            scratch((6, UNIT, HD), BF), scratch((6, UNIT, HD), BF),
            scratch((6, UNIT, HD), BF), scratch((6, UNIT, HD), BF),
            scratch(wide, BF), scratch(wide, BF), scratch((heads, UNIT)),
            scratch((UNIT, HD), BF), scratch((heads, NSTATE, HD)), dma((9,)),
            scratch((6, 3, 2, UNIT, HD), BF), scratch((6, 3, 2, UNIT, HD), BF),
            scratch((6, 3, 8, UNIT)), scratch((3, 3, 2, UNIT, HD), BF),
            scratch((5, UNIT, UNIT)), scratch((5, UNIT, UNIT)),
            scratch(wide), scratch(wide), scratch((HD, UNIT)), scratch((HD, UNIT)),
            scratch((HD, HD)), scratch((HD, HD)), scratch((UNIT, UNIT)), scratch((UNIT, UNIT)),
            scratch((UNIT, NSTATE)), scratch((UNIT, NSTATE)), scratch((UNIT, HD)), scratch((UNIT, HD)),
            scratch(wide), scratch((UNIT, NSTATE), BF), scratch((UNIT, NSTATE), BF), scratch((HD, UNIT)), scratch((HD, UNIT)),
            scratch((PLANE, heads + 1, *tile), BF), scratch((PLANE, heads + 1, *tile), BF),
            scratch((PLANE, heads, *tile)), scratch((PLANE, heads, *tile)),
            scratch((heads + 1, *tile), BF), scratch((ZS, heads + 1, *tile), BF),
            scratch((PLANE, heads, *tile), BF), scratch((PLANE, heads, *tile), BF),
            scratch((UNIT, HD)), scratch((4, UNIT // 4, HD)),
            scratch(tile), scratch((PLANE, *tile)), scratch(tile), scratch((ZS, *tile)),
            dma((2, 3, 2, 2)), dma((2, 3, 2, 2)), dma((2, 3)), dma((2, 3)), dma((2, 3)), dma((2, 3)),
            dma((2, 3)), dma((2, 3)), dma((3, 3, 2)), dma((3, 3, 2)),
            dma((7,)), dma((7,)), dma((7,)), dma((7,)), dma((7,)), dma((7,)),
            dma((3,)), dma((3,)), dma((7,)), dma((7,)), dma((7,)), dma((7,)),
        ],
        compiler_params=pltpu.CompilerParams(
            collective_id=0, has_side_effects=True, vmem_limit_bytes=60 * 1024 * 1024
        ),
    )(
        *by_head, step_sizes.T, decay_rates, skip_gains, bc_rows, saved_states[0]
    )
    dq6, dk6, dv6, gx, gst, gbc, gdec, gskip = finish(out)
    return (
        jnp.transpose(dq6, (1, 0, 2)),
        jnp.transpose(dk6, (1, 0, 2)),
        jnp.transpose(dv6, (1, 0, 2)),
        jnp.transpose(gx, (1, 0, 2)),
        gst.T,
        gbc,
        gdec[0],
        gskip[0],
    )


def solution(mesh):
    torus = Mesh(mesh.devices.reshape(ZS, XS, 2, mesh.shape["head"]), AXES)
    token_head = P(SEQ, "head", None)
    in_specs = (token_head,) * 6 + (
        P(SEQ, "head"), P("head"), P("head"), P(SEQ, None), P(SEQ, "head", None, None),
    )
    out_specs = (token_head,) * 4 + (P(SEQ, "head"), P(SEQ_HEAD, None), P("head"), P("head"))
    return jax.shard_map(shards, mesh=torus, in_specs=in_specs, out_specs=out_specs, check_vma=False)
```

```python
import functools
import math

import jax
import jax.numpy as jnp
from jax import lax
from jax.experimental import pallas as pl
from jax.experimental.pallas import tpu as pltpu
from jax.sharding import Mesh
from jax.sharding import PartitionSpec as P

NSTATE = 64
SEQ = ("seq_0", "seq_1", "seq_2")
SEQ_HEAD = ("seq_0", "seq_1", "seq_2", "head")
AXES = ("seq_0", "seq_1", "seq_2", "head")
MESH = pl.DeviceIdType.MESH
HIGHEST = lax.Precision.HIGHEST
NEG = -1e30
UNIT = 256
HD = 128
SCALE = HD**-0.5
SCALE2 = SCALE * math.log2(math.e)
PLANE = 8
ZS = 8
XS = 4
PAIRS = ZS * XS
BF = jnp.bfloat16
F32 = jnp.float32


def dot(a, b, dims, precision=None):
    return lax.dot_general(a, b, (dims, ((), ())), precision=precision, preferred_element_type=F32)


def nn(a, b, precision=None):
    return dot(a, b, ((1,), (0,)), precision)


def nt(a, b):
    return dot(a, b, ((1,), (1,)))


def tn(a, b):
    return dot(a, b, ((0,), (0,)))


def kernel(
    k6_in, v6_in, q6_in, g6_in, xs_in, dy_in, st_in, rates, skips, bc_in, s0_in,
    dq6, dk6, dv6, gx, gst, gbc, gdec, gskip,
    k6, v6, q6, g6, xs, dy, st, bc, s0, load_sem,
    kv, qg, stat, og, tscr, dscr,
    lb, sb, lrow, rrow, skr, whr, cbt, wsum, gb_acc, gc_acc, g0, ec,
    gdr, b_in, c_in, ldr, str_, car, plin, eplane, pplane, zt, zin, incout, inc,
    gbcl, gbin, tsrc, tpl, tz_src, tz,
    yin_s, yin_r, x1_s, x1_r, x2_s, x2_r, st_s, st_r, yo_s, yo_r,
    s1_s, s1_r, s2_s, s2_r, s3_s, s3_r, hb_s, hb_r, ta_s, ta_r, tb_s, tb_r,
):
    z, x, yh, hd = [lax.axis_index(a) for a in AXES]
    yl, core = hd // 2, hd % 2
    j = z * XS + x
    m = x * 2 + yh
    other = (1 - yl) * 2 + core
    heads = xs_in.shape[0]

    def at_pair(d):
        t = (j + d + PAIRS) % PAIRS
        return (t // XS, t % XS, yh, hd)

    def at_plane(mm):
        return (z, mm // 2, mm % 2, hd)

    def at_z(zz):
        return (zz, x, yh, hd)

    def at_head(hh):
        return (z, x, yh, hh)

    def at_y(k):
        return (z, x, k, other)

    def rcopy(src, dst, ss, rs, to):
        return pltpu.make_async_remote_copy(
            src_ref=src, dst_ref=dst, send_sem=ss, recv_sem=rs, device_id=to, device_id_type=MESH
        )

    peers = [at_y(0), at_y(1), at_pair(1), at_pair(-1), at_pair(2), at_pair(-2)]
    peers += [at_plane((m + o) % PLANE) for o in range(1, PLANE)]
    peers += [at_z((z + o) % ZS) for o in range(1, ZS)]
    peers += [at_head((hd + o) % 4) for o in range(1, 4)]
    loads = [
        pltpu.make_async_copy(src, dst, load_sem.at[n])
        for n, (src, dst) in enumerate(
            (
                (k6_in, k6), (v6_in, v6), (q6_in, q6), (g6_in, g6), (st_in, st),
                (bc_in, bc), (dy_in, dy), (xs_in, xs), (s0_in, s0),
            )
        )
    ]
    for load in loads:
        load.start()
    barrier = pltpu.get_barrier_semaphore()
    for p in peers:
        pl.semaphore_signal(barrier, inc=1, device_id=p, device_id_type=MESH)
    pl.semaphore_wait(barrier, len(peers))

    sources = ((k6, v6), (q6, g6))
    lands = ((kv, 4), (qg, 0))

    def y_in(h, w, t, k, sender):
        buf, base = lands[w]
        return rcopy(
            sources[w][t].at[3 * k + h], buf.at[base + sender, h, t],
            yin_s.at[w, h, t, k], yin_r.at[w, h, t, sender], at_y(k),
        )

    def start_y_in(h):
        for w in range(2):
            for t in range(2):
                for k in range(2):
                    y_in(h, w, t, k, yh).start()

    def wait_y_in(h, w):
        for t in range(2):
            for k in range(2):
                y_in(h, w, t, k, k).wait_recv()

    def hop(n, w, h):
        if w == 0:
            src, dst, to = (kv.at[pl.ds(6 - 2 * n, 2), h], kv.at[pl.ds(4 - 2 * n, 2), h], at_pair(1))
        else:
            src, dst, to = (qg.at[pl.ds(2 * n - 2, 2), h], qg.at[pl.ds(2 * n, 2), h], at_pair(-1))
        ss, rs = ((x1_s, x1_r), (x2_s, x2_r))[n - 1]
        return rcopy(src, dst, ss.at[w, h], rs.at[w, h], to)

    def stat_copy(h, d):
        return rcopy(
            stat.at[pl.ds(0, 2), h], stat.at[pl.ds(2 * d, 2), h],
            st_s.at[d - 1, h], st_r.at[d - 1, h], at_pair(-d),
        )

    outs = (dq6, dk6, dv6)

    def y_out(n, h, i, sender):
        return rcopy(
            og.at[n, h, i], outs[n].at[3 * sender + h],
            yo_s.at[n, h, i], yo_r.at[n, h, sender], at_y(i),
        )

    def s1(o, to_m, from_m):
        return rcopy(
            car.at[to_m], plin.at[from_m],
            s1_s.at[o - 1], s1_r.at[o - 1], at_plane(to_m),
        )

    def s2(o, to_z, from_z):
        return rcopy(zt, zin.at[from_z], s2_s.at[o - 1], s2_r.at[o - 1], at_z(to_z))

    def s3(o, to_m, from_m):
        return rcopy(
            incout.at[to_m], inc.at[from_m],
            s3_s.at[o - 1], s3_r.at[o - 1], at_plane(to_m),
        )

    def hb(o, to_h, from_h):
        return rcopy(
            gbcl.at[pl.ds(pl.multiple_of(64 * to_h, 64), 64), :], gbin.at[from_h],
            hb_s.at[o - 1], hb_r.at[o - 1], at_head(to_h),
        )

    def ta(o, to_m, from_m):
        return rcopy(tsrc, tpl.at[from_m], ta_s.at[o - 1], ta_r.at[o - 1], at_plane(to_m))

    def tb(o, to_z, from_z):
        return rcopy(tz_src, tz.at[from_z], tb_s.at[o - 1], tb_r.at[o - 1], at_z(to_z))

    def start_all(make, mine, count):
        for o in {4: (3, 1, 2), 8: (5, 3, 4, 7, 1, 6, 2) if mine is m else (4, 3, 5, 2, 6, 1, 7)}[count]:
            make(o, (mine + o) % count, mine).start()

    def recv_all(make, mine, count):
        for o in range(1, count):
            make(o, mine, (mine + count - o) % count).wait_recv()

    def sent_all(make, mine, count):
        for o in range(1, count):
            make(o, (mine + o) % count, mine).wait_send()

    rowi = lax.broadcasted_iota(jnp.int32, (UNIT, UNIT), 0)
    coli = lax.broadcasted_iota(jnp.int32, (UNIT, UNIT), 1)

    for load in loads[:4]:
        load.wait()
    start_y_in(0)
    for load in loads[4:]:
        load.wait()
    b_in[...] = bc[:, :NSTATE]
    c_in[...] = bc[:, NSTATE:]
    ldr[...] = jnp.zeros_like(ldr)
    str_[...] = jnp.zeros_like(str_)
    str_[0:heads, :] = st[...]
    for h in range(heads):
        ldr[h : h + 1, :] = st[h : h + 1, :] * rates[h]
    lrow[...] = nn(ldr[...], (rowi <= coli).astype(F32), HIGHEST)
    lcol = lrow[...].T
    steps = str_[...].T
    decays = jnp.exp(lcol[UNIT - 1 : UNIT, :])
    sublane = lax.broadcasted_iota(jnp.int32, (8, HD), 0)

    def as_terms(row):
        high = row.astype(BF).astype(F32)
        middle = (row - high).astype(BF).astype(F32)
        low = row - high - middle
        terms = jnp.where(sublane == 0, high, jnp.where(sublane == 1, middle, low))
        return jnp.where(sublane < 3, terms, 0.0).astype(BF)

    def from_terms(tile):
        return jnp.sum(tile.astype(F32), axis=0, keepdims=True)

    for h in range(heads):
        lb[h] = jnp.broadcast_to(lcol[:, h : h + 1], (UNIT, HD))
        sb[h] = jnp.broadcast_to(steps[:, h : h + 1], (UNIT, HD))

    def summary_of(h):
        scaled = (dy[h].astype(F32) * jnp.exp(lb[h])).astype(BF)
        part = tn(c_in[...], scaled)
        for i in range(PLANE):
            car[i, h] = part[8 * i : 8 * i + 8].astype(BF)

    def summary(n, carry):
        for i in range(3):
            summary_of(3 * n + i)
        return carry

    lax.fori_loop(0, heads // 3, summary, 0)
    decay_terms = as_terms(decays)
    for i in range(PLANE):
        car[i, heads] = decay_terms
    start_all(s1, m, PLANE)
    start_y_in(1)
    start_y_in(2)
    plin[m] = car[m]

    cbt[...] = nt(b_in[...], c_in[...])

    def send_own(h):
        for w in range(2):
            wait_y_in(h, w)
            hop(1, w, h).start()

    def send_next(h):
        for w in range(2):
            hop(1, w, h).wait_recv()
            hop(2, w, h).start()

    for ref in (rrow, skr, whr, wsum, gb_acc, gc_acc, g0, ec, tsrc):
        ref[...] = jnp.zeros_like(ref)
    lanes = lax.broadcasted_iota(jnp.int32, (UNIT, HD), 1)

    def wide(t):
        return jnp.concatenate([t, t], axis=1)

    def grads(h, carry):
        c_rows = c_in[...]
        lc, sc = (lb[h], sb[h])
        lr = lrow[pl.ds(h, 1), :]
        x_h, dy_h = (xs[h], dy[h])
        cb = cbt[...]
        decay = jnp.exp(jnp.where(coli >= rowi, lr - wide(lc), NEG))
        crossed = decay * nt(x_h, dy_h)
        weighted = crossed * wide(sc)
        wsum[...] += weighted
        rrow[pl.ds(h, 1), :] = jnp.sum(weighted * cb, axis=0, keepdims=True)
        paired = crossed * cb
        gdr[h] = nn((decay * cb).astype(BF), dy_h)
        early = nt(dy_h, s0[h].astype(BF)) * jnp.exp(lc)[:, :NSTATE]
        gc_acc[...] += early
        own = jnp.sum(paired[:, :HD] + paired[:, HD:], axis=1, keepdims=True)
        first = jnp.sum(early * c_rows.astype(F32), axis=1, keepdims=True)
        here = lanes == h
        g0[...] += jnp.where(here, own, 0.0)
        ec[...] += jnp.where(here, first, 0.0)
        skr[pl.ds(h, 1), :] = jnp.sum(dy_h.astype(F32) * x_h.astype(F32), axis=0, keepdims=True)
        return carry

    def carried_of(h):
        b_rows = b_in[...]
        lc, sc = (lb[h], sb[h])
        tail = jnp.exp(lc[UNIT - 1 : UNIT, :] - lc)
        inc_f = jnp.concatenate([inc[i, h].astype(F32) for i in range(PLANE)], axis=0)
        inc_h = inc_f.astype(BF)
        driven_grad = gdr[h] + tail * nn(b_rows, inc_h)
        gx[h] = (sc * driven_grad + skips[h] * dy[h].astype(F32)).astype(BF)
        late = nt(xs[h], inc_h) * tail[:, :NSTATE]
        gb_acc[...] += sc[:, :NSTATE] * late
        own = jnp.sum(late * b_rows.astype(F32), axis=1, keepdims=True)
        g0[...] += jnp.where(lanes == h, own, 0.0)
        whr[pl.ds(h, 1), :] = jnp.sum(inc_f * s0[h], axis=0, keepdims=True)

    def carried(n, carry):
        for i in range(2):
            carried_of(2 * n + i)
        return carry

    send_own(0)

    recv_all(s1, m, PLANE)
    acc = [jnp.zeros((8, HD), F32)] * heads
    prod = [jnp.ones((8, HD), F32)] * heads
    row_prod = jnp.ones((1, HD), F32)
    for mm in reversed(range(PLANE)):
        row = from_terms(plin[mm, heads])
        row_prod = row_prod * row
        for h in range(heads):
            eplane[mm, h] = acc[h]
            pplane[mm, h] = prod[h]
            decay = jnp.broadcast_to(row[:, h : h + 1], (8, HD))
            acc[h] = plin[mm, h].astype(F32) + decay * acc[h]
            prod[h] = prod[h] * decay
    for h in range(heads):
        zt[h] = acc[h].astype(BF)
    zt[heads] = as_terms(row_prod)
    start_all(s2, z, ZS)
    zin[z] = zt[...]

    send_own(1)
    send_next(0)
    send_own(2)
    lax.fori_loop(0, heads // 2, grads, 0)
    recv_all(s2, z, ZS)
    acc = [jnp.zeros((8, HD), F32)] * heads
    for zz in reversed(range(1, ZS)):
        row = from_terms(zin[zz, heads])
        for h in range(heads):
            decay = jnp.broadcast_to(row[:, h : h + 1], (8, HD))
            acc[h] = jnp.where(zz > z, zin[zz, h].astype(F32) + decay * acc[h], acc[h])
    for mm in range(PLANE):
        for h in range(heads):
            incout[mm, h] = (eplane[mm, h] + pplane[mm, h] * acc[h]).astype(BF)
    start_all(s3, m, PLANE)
    inc[m] = incout[m]

    send_next(1)
    lax.fori_loop(heads // 2, heads, grads, 0)

    def window(h):
        def block(i, carry):
            q, g = (qg[i, h, 0], qg[i, h, 1])
            top = None
            for u in range(5):
                s = nt(kv[i + u, h, 0], q) * SCALE2
                if u == 0:
                    s = jnp.where(rowi > coli, s, NEG)
                if u == 4:
                    s = jnp.where(rowi <= coli, s, NEG)
                else:
                    s = s + jnp.where(2 * j + i + u >= 4, 0.0, NEG)
                tscr[u] = s
                best = jnp.max(s, axis=0, keepdims=True)
                top = best if top is None else jnp.maximum(top, best)
            total = jnp.zeros((1, UNIT), F32)
            delta = jnp.zeros((1, UNIT), F32)
            for u in range(5):
                e = jnp.exp2(tscr[u] - top)
                dp = nt(kv[i + u, h, 1], g)
                total = total + jnp.sum(e, axis=0, keepdims=True)
                delta = delta + jnp.sum(e * dp, axis=0, keepdims=True)
                tscr[u] = e
                dscr[u] = dp
            inverse = 1.0 / total
            delta = delta * inverse
            out = jnp.zeros((HD, UNIT), F32)
            for u in range(5):
                ds = (tscr[u] * (dscr[u] - delta)).astype(BF)
                out = out + tn(kv[i + u, h, 0], ds)
            og[0, h, i] = (out * (inverse * SCALE)).T.astype(BF)
            stat[i, h, 0:1, :] = top + jnp.log2(total)
            stat[i, h, 1:2, :] = delta
            return carry

        lax.fori_loop(0, 2, block, 0)

    def key_pass(h):
        def block(i, carry):
            k, v = (kv[4 + i, h, 0], kv[4 + i, h, 1])
            dk = jnp.zeros((UNIT, HD), F32)
            dv = jnp.zeros((UNIT, HD), F32)
            for u in range(5):
                q, g = (qg[i + u, h, 0], qg[i + u, h, 1])
                s = nt(k, q) * SCALE2 - stat[i + u, h, 0:1, :]
                if u == 0:
                    s = jnp.where(coli >= rowi, s, NEG)
                else:
                    s = s + jnp.where(2 * j + i + u < 2 * PAIRS, 0.0, NEG)
                if u == 4:
                    s = jnp.where(coli < rowi, s, NEG)
                p = jnp.exp2(s)
                dv = dv + nn(p.astype(BF), g)
                ds = (p * (nt(v, g) - stat[i + u, h, 1:2, :])).astype(BF)
                dk = dk + nn(ds, q)
            og[1, h, i] = (dk * SCALE).astype(BF)
            og[2, h, i] = dv.astype(BF)
            return carry

        lax.fori_loop(0, 2, block, 0)

    def windows(h):
        hop(2, 0, h).wait_recv()
        window(h)
        for d in (2, 1):
            stat_copy(h, d).start()
        for i in range(2):
            y_out(0, h, i, yh).start()

    def keys(h):
        hop(2, 1, h).wait_recv()
        for d in (1, 2):
            stat_copy(h, d).wait_recv()
        key_pass(h)
        for n in (1, 2):
            for i in range(2):
                y_out(n, h, i, yh).start()

    for h in range(3):
        stat[0:2, h] = jnp.zeros((2, 8, UNIT), F32)
    windows(0)
    send_next(2)
    windows(1)
    keys(0)
    windows(2)

    recv_all(s3, m, PLANE)
    lax.fori_loop(0, heads // 2, carried, 0)
    w_all = wsum[...]
    gb_all = gb_acc[...] + nn(w_all, c_in[...].astype(F32), HIGHEST)
    gc_all = gc_acc[...] + nn(w_all.T, b_in[...].astype(F32), HIGHEST)
    gbcl[...] = jnp.concatenate([gb_all, gc_all], axis=1)
    start_all(hb, hd, 4)
    gbin[hd] = gbcl[pl.ds(pl.multiple_of(64 * hd, 64), 64), :]
    early_all = ec[...]
    change = steps * g0[...] - rrow[...].T - early_all
    strict = (coli < rowi).astype(F32)
    whole = decays * jnp.sum(whr[...].T, axis=0, keepdims=True)
    grad_log = nn(strict, change, HIGHEST) + (jnp.sum(early_all, axis=0, keepdims=True) + whole)
    own_rows, log_rows = (g0[...].T, grad_log.T)
    for h in range(heads):
        gst[h : h + 1, :] = own_rows[h : h + 1, :] + rates[h] * log_rows[h : h + 1, :]
    tsrc[0:1, :] = jnp.sum(steps * grad_log, axis=0, keepdims=True)
    tsrc[1:2, :] = jnp.sum(skr[...].T, axis=0, keepdims=True)
    start_all(ta, m, PLANE)
    tpl[m] = tsrc[...]

    keys(1)

    keys(2)

    recv_all(ta, m, PLANE)
    plane_sum = tpl[0]
    for mm in range(1, PLANE):
        plane_sum = plane_sum + tpl[mm]
    tz_src[...] = plane_sum
    start_all(tb, z, ZS)
    tz[z] = plane_sum
    recv_all(hb, hd, 4)
    gbc[...] = ((gbin[0] + gbin[1]) + gbin[2]) + gbin[3]
    recv_all(tb, z, ZS)
    total = tz[0]
    for zz in range(1, ZS):
        total = total + tz[zz]
    gdec[...] = total[0:1, :heads]
    gskip[...] = total[1:2, :heads]

    for h in range(3):
        for n in range(3):
            for i in range(2):
                y_out(n, h, i, i).wait_recv()
    for h in range(3):
        for w in range(2):
            for t in range(2):
                for k in range(2):
                    y_in(h, w, t, k, yh).wait_send()
            for n in (1, 2):
                hop(n, w, h).wait_send()
        for d in (1, 2):
            stat_copy(h, d).wait_send()
        for n in range(3):
            for i in range(2):
                y_out(n, h, i, yh).wait_send()
    sent_all(s1, m, PLANE)
    sent_all(s2, z, ZS)
    sent_all(s3, m, PLANE)
    sent_all(hb, hd, 4)
    sent_all(ta, m, PLANE)
    sent_all(tb, z, ZS)


def finish_kernel(*refs):
    count = len(refs) // 2
    sems = refs[-1]
    copies = [
        pltpu.make_async_copy(refs[n], refs[count + n], sems.at[n]) for n in range(count)
    ]
    for copy in copies:
        copy.start()
    for copy in copies:
        copy.wait()


def finish(arrays):
    count = len(arrays)
    return pl.pallas_call(
        finish_kernel,
        name="finish",
        out_shape=[jax.ShapeDtypeStruct(a.shape, a.dtype) for a in arrays],
        in_specs=[pl.BlockSpec(memory_space=pltpu.VMEM)] * count,
        out_specs=[pl.BlockSpec(memory_space=pl.ANY)] * count,
        scratch_shapes=[pltpu.SemaphoreType.DMA((count,))],
    )(*[pltpu.with_memory_space_constraint(a, pltpu.VMEM) for a in arrays])


def shards(
    queries, key_vectors, values, out_grad, ssm_input, ssm_out_grad,
    step_sizes, decay_rates, skip_gains, bc_rows, saved_states,
):
    heads = ssm_input.shape[1]
    by_head = [
        jnp.transpose(t, (1, 0, 2))
        for t in (key_vectors, values, queries, out_grad, ssm_input, ssm_out_grad)
    ]
    vmem = pl.BlockSpec(memory_space=pltpu.VMEM)
    hbm = pl.BlockSpec(memory_space=pl.ANY)
    smem = pl.BlockSpec(memory_space=pltpu.SMEM)

    def kept(s, t=F32):
        return pltpu.VMEM(s, t)

    def scratch(s, t=F32):
        return pltpu.VMEM(s, t)

    dma = pltpu.SemaphoreType.DMA
    wide = (heads, UNIT, HD)
    tile = (8, HD)
    out = pl.pallas_call(
        kernel,
        name="mixers",
        out_shape=[
            kept((6, UNIT, HD), BF), kept((6, UNIT, HD), BF), kept((6, UNIT, HD), BF),
            kept(wide, BF), kept((heads, UNIT)), kept((UNIT // 4, HD)),
            kept((1, heads)), kept((1, heads)),
        ],
        in_specs=[hbm] * 7 + [smem] * 2 + [hbm] * 2,
        out_specs=[vmem] * 8,
        scratch_shapes=[
            scratch((6, UNIT, HD), BF), scratch((6, UNIT, HD), BF),
            scratch((6, UNIT, HD), BF), scratch((6, UNIT, HD), BF),
            scratch(wide, BF), scratch(wide, BF), scratch((heads, UNIT)),
            scratch((UNIT, HD), BF), scratch((heads, NSTATE, HD)), dma((9,)),
            scratch((6, 3, 2, UNIT, HD), BF), scratch((6, 3, 2, UNIT, HD), BF),
            scratch((6, 3, 8, UNIT)), scratch((3, 3, 2, UNIT, HD), BF),
            scratch((5, UNIT, UNIT)), scratch((5, UNIT, UNIT)),
            scratch(wide), scratch(wide), scratch((HD, UNIT)), scratch((HD, UNIT)),
            scratch((HD, HD)), scratch((HD, HD)), scratch((UNIT, UNIT)), scratch((UNIT, UNIT)),
            scratch((UNIT, NSTATE)), scratch((UNIT, NSTATE)), scratch((UNIT, HD)), scratch((UNIT, HD)),
            scratch(wide), scratch((UNIT, NSTATE), BF), scratch((UNIT, NSTATE), BF), scratch((HD, UNIT)), scratch((HD, UNIT)),
            scratch((PLANE, heads + 1, *tile), BF), scratch((PLANE, heads + 1, *tile), BF),
            scratch((PLANE, heads, *tile)), scratch((PLANE, heads, *tile)),
            scratch((heads + 1, *tile), BF), scratch((ZS, heads + 1, *tile), BF),
            scratch((PLANE, heads, *tile), BF), scratch((PLANE, heads, *tile), BF),
            scratch((UNIT, HD)), scratch((4, UNIT // 4, HD)),
            scratch(tile), scratch((PLANE, *tile)), scratch(tile), scratch((ZS, *tile)),
            dma((2, 3, 2, 2)), dma((2, 3, 2, 2)), dma((2, 3)), dma((2, 3)), dma((2, 3)), dma((2, 3)),
            dma((2, 3)), dma((2, 3)), dma((3, 3, 2)), dma((3, 3, 2)),
            dma((7,)), dma((7,)), dma((7,)), dma((7,)), dma((7,)), dma((7,)),
            dma((3,)), dma((3,)), dma((7,)), dma((7,)), dma((7,)), dma((7,)),
        ],
        compiler_params=pltpu.CompilerParams(
            collective_id=0, has_side_effects=True, vmem_limit_bytes=60 * 1024 * 1024
        ),
    )(
        *by_head, step_sizes.T, decay_rates, skip_gains, bc_rows, saved_states[0]
    )
    dq6, dk6, dv6, gx, gst, gbc, gdec, gskip = finish(out)
    return (
        jnp.transpose(dq6, (1, 0, 2)),
        jnp.transpose(dk6, (1, 0, 2)),
        jnp.transpose(dv6, (1, 0, 2)),
        jnp.transpose(gx, (1, 0, 2)),
        gst.T,
        gbc,
        gdec[0],
        gskip[0],
    )


def solution(mesh):
    torus = Mesh(mesh.devices.reshape(ZS, XS, 2, mesh.shape["head"]), AXES)
    token_head = P(SEQ, "head", None)
    in_specs = (token_head,) * 6 + (
        P(SEQ, "head"), P("head"), P("head"), P(SEQ, None), P(SEQ, "head", None, None),
    )
    out_specs = (token_head,) * 4 + (P(SEQ, "head"), P(SEQ_HEAD, None), P("head"), P("head"))
    return jax.shard_map(shards, mesh=torus, in_specs=in_specs, out_specs=out_specs, check_vma=False)
```
